32 devices in a mesh: dp: 2 (over x), ffn: 4 (over z), emb: 4 (over y, core).
Axes of the slice: x: 2, y: 2, z: 4, core: 2. Of those that a mesh axis runs over, the one named last changes fastest.
Arguments:
- hidden: bfloat16 [256, 2048], P('dp', 'emb'), parts along dimension 0
- norm_pre: bfloat16 [2048], P('emb')
- norm_post: bfloat16 [2048], P('emb')
- w_router: bfloat16 [2048, 128], P('emb')
- w_gate: bfloat16 [128, 2048, 768], P(None, 'emb', 'ffn')
- w_up: bfloat16 [128, 2048, 768], P(None, 'emb', 'ffn')
- w_down: bfloat16 [128, 768, 2048], P(None, 'ffn', 'emb')
- choice: int32 [256, 8], P('dp'), parts along dimension 0
Outputs:
- output: bfloat16 [256, 2048], P('dp', 'emb'), parts along dimension 0
There are 2 independent parts. The reference program is written for one: setup_inputs(seed, part) draws one part's arguments, and reference() takes and returns one part's arrays. A program takes and returns all parts, laid end to end along the dimension named above; an argument that names none is the same for every part.
All inputs are finite; a program needn't handle non-finite values.
Results may differ from the reference program's by a relative error of at most 0.0119329.
Values are sent between devices in bfloat16 or wider.
A program may use at most 1 GiB of HBM per device.

```python
import math
import jax
import jax.numpy as jnp
from jax import lax

D = 2048
E = 128
F = 768
TOP = 8
B = 128
CAP = 2 * B * TOP // E
EPS = 1e-5


def width_profile(key, size):
    slope = jax.random.uniform(key, (), minval=1.5, maxval=2.5)
    return jnp.exp(slope * (jnp.arange(size, dtype=jnp.float32) / size - 0.5))


def draw_choice(key):
    key_hot, key_perm, key_score = jax.random.split(key, 3)
    hot_id = jax.random.randint(key_hot, (), 0, E)
    forced = jax.random.permutation(key_perm, B) < (3 * B) // 4
    expert_ids = jnp.arange(E)
    score = jax.random.randint(key_score, (B, E), 1, 1048576) * E + expert_ids[None, :]
    score = jnp.where(forced[:, None] & (expert_ids[None, :] == hot_id), 0, score)
    return jnp.argsort(score, axis=1, stable=True)[:, :TOP].astype(jnp.int32)


def setup_inputs(seed: int = 0, part: int = 0) -> dict:
    base_key = jax.random.key(seed)
    part_keys = jax.random.split(jax.random.fold_in(base_key, part), 4)
    shared_keys = jax.random.split(base_key, 7)
    row_scale = jnp.exp(0.5 * jax.random.normal(part_keys[0], (B, 1)))
    hidden = jax.random.normal(part_keys[1], (B, D)) * row_scale * width_profile(part_keys[2], D)[None, :]
    norm_pre = 1.0 + 0.3 * jax.random.normal(shared_keys[0], (D,))
    norm_post = 1.0 + 0.3 * jax.random.normal(shared_keys[1], (D,))
    w_router = jax.random.normal(shared_keys[2], (D, E)) * (1.5 / math.sqrt(D))
    w_gate = jax.random.normal(shared_keys[3], (E, D, F)) * (1.0 / math.sqrt(D))
    w_up = jax.random.normal(shared_keys[4], (E, D, F)) * (1.0 / math.sqrt(D))
    w_down = jax.random.normal(shared_keys[5], (E, F, D)) * (1.0 / math.sqrt(F)) * width_profile(shared_keys[6], D)[None, None, :]
    return {
        'hidden': hidden.astype(jnp.bfloat16),
        'norm_pre': norm_pre.astype(jnp.bfloat16),
        'norm_post': norm_post.astype(jnp.bfloat16),
        'w_router': w_router.astype(jnp.bfloat16),
        'w_gate': w_gate.astype(jnp.bfloat16),
        'w_up': w_up.astype(jnp.bfloat16),
        'w_down': w_down.astype(jnp.bfloat16),
        'choice': draw_choice(part_keys[3]),
    }


def route_tokens(choice, router_prob):
    onehot = (choice[:, :, None] == jnp.arange(E)[None, None, :]).astype(jnp.int32)
    assigned = jnp.sum(onehot, axis=1)
    before = jnp.cumsum(assigned, axis=0) - assigned
    slot_idx = jnp.sum(onehot * before[:, None, :], axis=2)
    position = jnp.where(slot_idx < CAP, choice * CAP + slot_idx, E * CAP)
    gate_val = jnp.take_along_axis(router_prob, choice, axis=1)
    flat_pos = position.reshape(-1)
    token_ids = jnp.repeat(jnp.arange(B, dtype=jnp.int32), TOP)
    slot_token = jnp.full((E * CAP,), B, jnp.int32).at[flat_pos].set(token_ids, mode='drop')
    slot_gate = jnp.zeros((E * CAP,), jnp.float32).at[flat_pos].set(gate_val.reshape(-1), mode='drop')
    return position, slot_token, slot_gate


def expert_ffn(operands):
    slot_rows, gate_w, up_w, down_w = operands
    z_gate = jnp.dot(slot_rows, gate_w, preferred_element_type=jnp.float32).astype(jnp.bfloat16)
    z_up = jnp.dot(slot_rows, up_w, preferred_element_type=jnp.float32).astype(jnp.bfloat16)
    act_val = (jax.nn.gelu(z_gate.astype(jnp.float32), approximate=True) * z_up.astype(jnp.float32)).astype(jnp.bfloat16)
    return jnp.dot(act_val, down_w, preferred_element_type=jnp.float32).astype(jnp.bfloat16)


def reference(hidden, norm_pre, norm_post, w_router, w_gate, w_up, w_down, choice):
    hid_f32 = hidden.astype(jnp.float32)
    inv_pre = lax.rsqrt(jnp.mean(hid_f32 * hid_f32, axis=1, keepdims=True) + EPS)
    normed = (hid_f32 * inv_pre * norm_pre.astype(jnp.float32)).astype(jnp.bfloat16)
    logits = jnp.dot(normed, w_router, preferred_element_type=jnp.float32)
    router_prob = jax.nn.softmax(logits, axis=1)
    position, slot_token, slot_gate = route_tokens(choice, router_prob)
    expert_in = jnp.take(normed, slot_token, axis=0, mode='fill', fill_value=0).reshape(E, CAP, D)
    expert_out = lax.map(expert_ffn, (expert_in, w_gate, w_up, w_down))
    weighted = (expert_out.reshape(E * CAP, D).astype(jnp.float32) * slot_gate[:, None]).astype(jnp.bfloat16)
    picked = jnp.take(weighted, position, axis=0, mode='fill', fill_value=0)
    mix_sum = jnp.sum(picked.astype(jnp.float32), axis=1)
    inv_post = lax.rsqrt(jnp.mean(mix_sum * mix_sum, axis=1, keepdims=True) + EPS)
    return (hid_f32 + mix_sum * inv_post * norm_post.astype(jnp.float32)).astype(jnp.bfloat16)
```

```python
import functools

import jax
import jax.numpy as jnp
from jax import lax
from jax.experimental import pallas as pl
from jax.experimental.pallas import tpu as pltpu
from jax.sharding import PartitionSpec as P

EPS = 1e-5
MESH = pl.DeviceIdType.MESH
BF = jnp.bfloat16
F32 = jnp.float32
RING = 6
EB = 8
CAP = 16
NB = 16


def remote(src, dst, send, recv, **where):
    return pltpu.make_async_remote_copy(
        src_ref=src, dst_ref=dst, send_sem=send, recv_sem=recv,
        device_id=where, device_id_type=MESH)


def kernel(model_width, h_ref, pre_ref, post_ref, wr_ref, choice_ref, w0_ref, w1_ref, w2_ref, o_ref,
           ring, w2buf, oht, oh, bnorm, zsend, recv1, snd2, recv2, own2, gall, pos_ref, pt_ref,
           lbuf, lrecv1, lsnd2, lrecv2, pbuf, sq_snd, sq_recv, macc, ubuf, mrecv, mown, tq_snd, tq_recv, obuf,
           ring_sem, w2_sem, s1_s, s1_r, s2_s, s2_r, gy_s, gy_r, gp_s, gp_r, gf_s, gf_r,
           l_s, l_r, sq_s, sq_r, rs_s, rs_r, tq_s, tq_r, ag_s, ag_r):
    ffn = lax.axis_index("ffn")
    emb = lax.axis_index("emb")
    core = emb % 2
    row = emb // 2
    partner = emb + 1 - 2 * core
    across = (emb + 2) % 4
    tok = h_ref.shape[0]
    half = EB * CAP // 2
    quarter = half // 2
    ROWS = EB * CAP

    def ring_copies(batch):
        slot = batch % RING
        e0 = pl.ds(batch * EB, EB)
        return [
            pltpu.make_async_copy(w0_ref.at[e0, pl.ds(0, 128)], ring.at[slot, :, pl.ds(0, 128)], ring_sem.at[slot, 0]),
            pltpu.make_async_copy(w1_ref.at[e0, pl.ds(0, 128)], ring.at[slot, :, pl.ds(128, 128)], ring_sem.at[slot, 1]),
            pltpu.make_async_copy(w0_ref.at[e0, pl.ds(128, 64)], ring.at[slot, :, pl.ds(256, 64)], ring_sem.at[slot, 2]),
            pltpu.make_async_copy(w1_ref.at[e0, pl.ds(128, 64)], ring.at[slot, :, pl.ds(320, 64)], ring_sem.at[slot, 3]),
        ]

    def w2_copy(batch):
        e0 = pl.ds(batch * EB, EB)
        return pltpu.make_async_copy(w2_ref.at[e0], w2buf.at[e0], w2_sem.at[batch])

    for b in range(RING):
        for c in ring_copies(b):
            c.start()

    hf = h_ref[...].astype(F32)
    sq = jnp.sum(hf * hf, axis=1, keepdims=True)
    sq_rows = jnp.transpose(jnp.broadcast_to(sq, (tok, tok)))
    sq_snd[...] = sq_rows[0:8]

    barrier = pltpu.get_barrier_semaphore()
    for d in range(1, 4):
        pl.semaphore_signal(barrier, inc=1, device_id={"emb": (emb + d) % 4}, device_id_type=MESH)
        pl.semaphore_signal(barrier, inc=1, device_id={"ffn": (ffn + d) % 4}, device_id_type=MESH)
    pl.semaphore_wait(barrier, 6)

    def sq_copy(d):
        return remote(sq_snd, sq_recv.at[d - 1], sq_s.at[d - 1], sq_r.at[d - 1], emb=(emb + d) % 4)

    for d in range(1, 4):
        sq_copy(d).start()

    experts = lax.broadcasted_iota(jnp.int32, (tok, tok), 0)
    lanes = lax.broadcasted_iota(jnp.int32, (tok, tok), 1)
    assigned = jnp.zeros((tok, tok), F32)
    for k in range(choice_ref.shape[0]):
        assigned = assigned + (jnp.broadcast_to(choice_ref[k:k + 1, :], (tok, tok)) == experts).astype(F32)
    upper = (experts < lanes).astype(F32).astype(BF)
    before = jnp.dot(assigned.astype(BF), upper, preferred_element_type=F32)
    pos_ref[...] = jnp.where(assigned > 0.5, before, 1000.0)
    slot_no = lax.broadcasted_iota(jnp.int32, (CAP, tok), 0).astype(F32)

    def build(b, carry):
        rows = pos_ref[pl.ds(pl.multiple_of(b * EB, EB), EB), :]
        hot = jnp.concatenate(
            [(jnp.broadcast_to(rows[e:e + 1, :], (CAP, tok)) == slot_no).astype(F32) for e in range(EB)], axis=0)
        oht[b] = hot.astype(BF)
        oh[b] = jnp.transpose(hot).astype(BF)
        return carry

    lax.fori_loop(0, NB, build, 0)

    total = sq_snd[...]
    for d in range(1, 4):
        sq_copy(d).wait_recv()
    for d in range(1, 4):
        total = total + sq_recv[d - 1]
    inv_rows = lax.rsqrt(total / model_width + EPS)
    inv = jnp.transpose(jnp.broadcast_to(inv_rows[0:1, :], (tok, tok)))[:, 0:1]
    bnorm[...] = (h_ref[...].astype(F32) * inv * pre_ref[...].astype(F32)).astype(BF)

    lbuf[...] = jnp.dot(bnorm[...], wr_ref[...], preferred_element_type=F32)
    htok = tok // 2
    mine = pl.ds(pl.multiple_of(core * htok, htok), htok)

    def logit_pair():
        return remote(lbuf, lrecv1, l_s.at[0], l_r.at[0], emb=partner)

    def logit_across():
        return remote(lsnd2, lrecv2, l_s.at[1], l_r.at[1], emb=across)

    def prob_pair():
        return remote(pbuf.at[mine], pbuf.at[mine], l_s.at[2], l_r.at[2], emb=partner)

    logit_pair().start()

    def z_pair(j):
        return remote(zsend.at[j, pl.ds(pl.multiple_of((1 - core) * half, half), half)], recv1.at[j],
                      s1_s.at[j], s1_r.at[j], emb=partner)

    def z_across(j):
        return remote(snd2.at[j], recv2.at[j], s2_s.at[j], s2_r.at[j], emb=across)

    own_rows = pl.ds(pl.multiple_of(core * half + row * quarter, quarter), quarter)
    other_rows = pl.ds(pl.multiple_of(core * half + (1 - row) * quarter, quarter), quarter)

    def g_across(k):
        return remote(gall.at[k, own_rows], gall.at[k, own_rows], gy_s.at[k], gy_r.at[k], emb=across)

    def g_pair(k):
        return remote(gall.at[k, own_rows], gall.at[k, own_rows], gp_s.at[k], gp_r.at[k], emb=partner)

    def g_forward(k):
        return remote(gall.at[k, other_rows], gall.at[k, other_rows], gf_s.at[k], gf_r.at[k], emb=partner)

    macc[...] = jnp.zeros_like(macc)

    def step(i, carry):
        @pl.when(i < NB)
        def _():
            slot = i % RING
            for c in ring_copies(i):
                c.wait()
            x = jnp.dot(oht[i], bnorm[...], preferred_element_type=F32).astype(BF)
            for e in range(EB):
                z = lax.dot_general(x[e * CAP:(e + 1) * CAP], ring[slot, e], (((1,), (1,)), ((), ())),
                                    preferred_element_type=F32)
                zsend[i, e * CAP:(e + 1) * CAP, :] = z.astype(BF)
            z_pair(i).start()

            @pl.when(i + RING < NB)
            def _():
                for c in ring_copies(i + RING):
                    c.start()
            w2_copy(i).start()

        @pl.when((i >= 1) & (i < NB + 1))
        def _():
            j = i - 1
            z_pair(j).wait_recv()
            snd2[j] = (zsend[j, other_rows, :].astype(F32)
                       + recv1[j, pl.ds(pl.multiple_of((1 - row) * quarter, quarter), quarter), :].astype(F32)).astype(BF)
            z_across(j).start()
            own2[j] = (zsend[j, own_rows, :].astype(F32)
                       + recv1[j, pl.ds(pl.multiple_of(row * quarter, quarter), quarter), :].astype(F32))

        @pl.when((i >= 3) & (i < NB + 3))
        def _():
            k = i - 3
            z_across(k).wait_recv()
            z = (own2[k] + recv2[k].astype(F32)).astype(BF).astype(F32)
            low = jax.nn.gelu(z[:, 0:128], approximate=True) * z[:, 128:256]
            mixed = z[:, 256:384]
            high = jax.nn.gelu(mixed, approximate=True) * pltpu.roll(mixed, 64, 1)
            gall[k, own_rows, 0:128] = low.astype(BF)
            gall[k, own_rows, 128:256] = high.astype(BF)
            g_across(k).start()
            g_pair(k).start()

        @pl.when((i >= 5) & (i < NB + 5))
        def _():
            g_across(i - 5).wait_recv()
            g_forward(i - 5).start()

        @pl.when(i == 2)
        def _():
            logit_pair().wait_recv()
            lbuf2 = lbuf[mine, :] + lrecv1[mine, :]
            lsnd2[...] = lbuf2
            logit_across().start()

        @pl.when(i == 5)
        def _():
            logit_across().wait_recv()
            logits = lsnd2[...] + lrecv2[...]
            pbuf[mine, :] = jax.nn.softmax(logits, axis=1)
            prob_pair().start()

        @pl.when(i == 8)
        def _():
            prob_pair().wait_recv()
            pt_ref[...] = jnp.transpose(pbuf[...])

        @pl.when(i >= NB)
        def _():
            b = i - NB
            w2_copy(b).wait()
            g_pair(b).wait_recv()
            g_forward(b).wait_recv()
            probs = pt_ref[pl.ds(pl.multiple_of(b * EB, EB), EB), :]
            for e in range(EB):
                rows = slice(e * CAP, (e + 1) * CAP)
                y = jnp.dot(gall[b, rows, 0:192], w2buf[b * EB + e], preferred_element_type=F32)
                gate = jnp.sum(oht[b, rows, :].astype(F32) * probs[e:e + 1, :], axis=1, keepdims=True)
                ubuf[rows, :] = (y.astype(BF).astype(F32) * gate).astype(BF)
            macc[...] += jnp.dot(oh[b], ubuf[...], preferred_element_type=F32)
        return carry

    lax.fori_loop(0, 2 * NB, step, 0)

    part = tok // 4

    def rs_copy(d):
        peer = (ffn + d) % 4
        return remote(macc.at[pl.ds(pl.multiple_of(peer * part, part), part)], mrecv.at[d - 1],
                      rs_s.at[d - 1], rs_r.at[d - 1], ffn=peer)

    for d in (2, 1, 3):
        rs_copy(d).start()
    my_tok = pl.ds(pl.multiple_of(ffn * part, part), part)
    m = macc[my_tok, :]

    def drain(j, carry):
        z_pair(j).wait_send()
        z_across(j).wait_send()
        g_across(j).wait_send()
        g_pair(j).wait_send()
        g_forward(j).wait_send()
        return carry

    lax.fori_loop(0, NB, drain, 0)
    logit_pair().wait_send()
    logit_across().wait_send()
    prob_pair().wait_send()
    for d in range(1, 4):
        sq_copy(d).wait_send()
        rs_copy(d).wait_recv()
    for d in range(1, 4):
        m = m + mrecv[d - 1]
    mown[...] = m
    m2 = m * m
    tq_snd[...] = m2[:, 0:128] + m2[:, 128:256] + m2[:, 256:384] + m2[:, 384:512]

    def tq_copy(d):
        return remote(tq_snd, tq_recv.at[d - 1], tq_s.at[d - 1], tq_r.at[d - 1], emb=(emb + d) % 4)

    for d in range(1, 4):
        tq_copy(d).start()
    for d in range(1, 4):
        rs_copy(d).wait_send()
        tq_copy(d).wait_recv()
    tot = tq_snd[...]
    for d in range(1, 4):
        tot = tot + tq_recv[d - 1]
    inv_post = lax.rsqrt(jnp.sum(tot, axis=1, keepdims=True) / model_width + EPS)
    res = h_ref[my_tok, :].astype(F32) + mown[...] * inv_post * post_ref[...].astype(F32)
    obuf[my_tok, :] = res.astype(BF)

    def ag_copy(d):
        return remote(obuf.at[my_tok], obuf.at[my_tok], ag_s.at[d - 1], ag_r.at[d - 1], ffn=(ffn + d) % 4)

    for d in (2, 1, 3):
        ag_copy(d).start()
    for d in range(1, 4):
        tq_copy(d).wait_send()
        ag_copy(d).wait_recv()
    o_ref[...] = obuf[...]
    for d in range(1, 4):
        ag_copy(d).wait_send()


def solution(mesh):
    emb_size = mesh.shape['emb']

    def local_block(hidden, norm_pre, norm_post, w_router, w_gate, w_up, w_down, choice):
        tok, width = hidden.shape
        experts, _, fw = w_gate.shape
        dma = pltpu.SemaphoreType.DMA
        vm = pltpu.VMEM
        rows = EB * CAP
        vspec = pl.BlockSpec(memory_space=pltpu.VMEM)
        hspec = pl.BlockSpec(memory_space=pl.ANY)
        return pl.pallas_call(
            functools.partial(kernel, width * emb_size),
            out_shape=jax.ShapeDtypeStruct((tok, width), BF),
            in_specs=[vspec] * 5 + [hspec] * 3,
            out_specs=vspec,
            scratch_shapes=[
                vm((RING, EB, 2 * fw, width), BF), vm((experts, fw, width), BF),
                vm((NB, rows, tok), BF), vm((NB, tok, rows), BF), vm((tok, width), BF),
                vm((NB, rows, 2 * fw), BF), vm((NB, rows // 2, 2 * fw), BF),
                vm((NB, rows // 4, 2 * fw), BF), vm((NB, rows // 4, 2 * fw), BF), vm((NB, rows // 4, 2 * fw), F32),
                vm((NB, rows, 256), BF), vm((experts, tok), F32), vm((experts, tok), F32),
                vm((tok, experts), F32), vm((tok, experts), F32), vm((tok // 2, experts), F32),
                vm((tok // 2, experts), F32), vm((tok, experts), F32),
                vm((8, tok), F32), vm((3, 8, tok), F32),
                vm((tok, width), F32), vm((rows, width), BF), vm((3, tok // 4, width), F32), vm((tok // 4, width), F32),
                vm((tok // 4, 128), F32), vm((3, tok // 4, 128), F32), vm((tok, width), BF),
                dma((RING, 4)), dma((NB,)),
                dma((NB,)), dma((NB,)), dma((NB,)), dma((NB,)), dma((NB,)), dma((NB,)),
                dma((NB,)), dma((NB,)), dma((NB,)), dma((NB,)),
                dma((3,)), dma((3,)), dma((3,)), dma((3,)), dma((3,)), dma((3,)), dma((3,)), dma((3,)), dma((3,)), dma((3,)),
            ],
            compiler_params=pltpu.CompilerParams(
                collective_id=0, has_side_effects=True, vmem_limit_bytes=67043328),
        )(hidden, norm_pre.reshape(1, width), norm_post.reshape(1, width), w_router, choice.T,
          jnp.swapaxes(w_gate, 1, 2), jnp.swapaxes(w_up, 1, 2), w_down)

    in_specs = (P('dp', 'emb'), P('emb'), P('emb'), P('emb', None), P(None, 'emb', 'ffn'), P(None, 'emb', 'ffn'), P(None, 'ffn', 'emb'), P('dp', None))
    return jax.shard_map(local_block, mesh=mesh, in_specs=in_specs, out_specs=P('dp', 'emb'), check_vma=False)
```

```python
import functools

import jax
import jax.numpy as jnp
from jax import lax
from jax.experimental import pallas as pl
from jax.experimental.pallas import tpu as pltpu
from jax.sharding import PartitionSpec as P

EPS = 1e-5
MESH = pl.DeviceIdType.MESH
BF = jnp.bfloat16
F32 = jnp.float32
EB = 8
CAP = 16
NB = 16
RING = 6
EARLY = 4
LAG_C, LAG_D = 3, 6


def remote(src, dst, send, recv, **where):
    return pltpu.make_async_remote_copy(
        src_ref=src, dst_ref=dst, send_sem=send, recv_sem=recv,
        device_id=where, device_id_type=MESH)


def kernel(model_width, h_hbm, pre_hbm, post_hbm, wr_hbm, choice_hbm, w0_ref, w1_ref, w2_ref, o_ref,
           h_ref, pre_ref, post_ref, wr_ref, choice_ref,
           ring, w2buf, oht, oh, bnorm, zsend, recv1, snd2, recv2, own2, gall, pos_ref, pt_ref,
           lbuf, lrecv1, lsnd2, lrecv2, pbuf, sq_snd, sq_recv, macc, ubuf, mrecv, mown, tq_snd, tq_recv, obuf, xbuf,
           in_sem, ring_sem, w2_sem, snd_sem, s1_r, s2_r, gy_r, gp_r, gf_r,
           l_s, l_r, sq_s, sq_r, rs_s, rs_r, tq_s, tq_r, ag_s, ag_r):
    ffn = lax.axis_index("ffn")
    emb = lax.axis_index("emb")
    core = emb % 2
    row = emb // 2
    partner = emb + 1 - 2 * core
    across = (emb + 2) % 4
    tok, width = h_ref.shape
    half = EB * CAP // 2
    quarter = half // 2

    barrier = pltpu.get_barrier_semaphore()
    for d in range(1, 4):
        pl.semaphore_signal(barrier, inc=1, device_id={"emb": (emb + d) % 4}, device_id_type=MESH)
        pl.semaphore_signal(barrier, inc=1, device_id={"ffn": (ffn + d) % 4}, device_id_type=MESH)

    loads = [pltpu.make_async_copy(a, b, in_sem.at[n]) for n, (a, b) in enumerate(
        [(h_hbm, h_ref), (choice_hbm, choice_ref), (pre_hbm, pre_ref), (wr_hbm, wr_ref), (post_hbm, post_ref)])]
    for c in loads:
        c.start()

    def ring_copies(batch):
        slot = batch % RING
        e0 = pl.ds(batch * EB, EB)
        return [
            pltpu.make_async_copy(w0_ref.at[e0, pl.ds(0, 128)], ring.at[slot, :, pl.ds(0, 128)], ring_sem.at[slot, 0]),
            pltpu.make_async_copy(w1_ref.at[e0, pl.ds(0, 128)], ring.at[slot, :, pl.ds(128, 128)], ring_sem.at[slot, 1]),
            pltpu.make_async_copy(w0_ref.at[e0, pl.ds(128, 64)], ring.at[slot, :, pl.ds(256, 64)], ring_sem.at[slot, 2]),
            pltpu.make_async_copy(w1_ref.at[e0, pl.ds(128, 64)], ring.at[slot, :, pl.ds(320, 64)], ring_sem.at[slot, 3]),
        ]

    def w2_copy(pair):
        e0 = pl.ds(pair * 2 * EB, 2 * EB)
        return pltpu.make_async_copy(w2_ref.at[e0], w2buf.at[e0], w2_sem.at[pair])

    loads[0].wait()
    for c in loads[1:]:
        c.wait()
    for b in range(RING):
        for c in ring_copies(b):
            c.start()
    for b in range(EARLY):
        w2_copy(b).start()

    hf = h_ref[...].astype(F32)
    sq = jnp.sum(hf * hf, axis=1, keepdims=True)
    sq_snd[...] = jnp.transpose(jnp.broadcast_to(sq, (tok, tok)))[0:8]

    pl.semaphore_wait(barrier, 6)

    def sq_copy(d):
        return remote(sq_snd, sq_recv.at[d - 1], sq_s.at[d - 1], sq_r.at[d - 1], emb=(emb + d) % 4)

    for d in (2, 3, 1):
        sq_copy(d).start()

    experts = lax.broadcasted_iota(jnp.int32, (tok, tok), 0)
    lanes = lax.broadcasted_iota(jnp.int32, (tok, tok), 1)
    assigned = jnp.zeros((tok, tok), F32)
    for k in range(choice_ref.shape[0]):
        assigned = assigned + (jnp.broadcast_to(choice_ref[k:k + 1, :], (tok, tok)) == experts).astype(F32)
    upper = (experts < lanes).astype(F32).astype(BF)
    before = jnp.dot(assigned.astype(BF), upper, preferred_element_type=F32)
    pos_ref[...] = jnp.where(assigned > 0.5, before, 1000.0)
    slot_no = lax.broadcasted_iota(jnp.int32, (CAP, tok), 0).astype(F32)

    def build(b, carry):
        rows = pos_ref[pl.ds(pl.multiple_of(b * 2 * EB, 2 * EB), 2 * EB), :]
        hot = jnp.concatenate(
            [(jnp.broadcast_to(rows[e:e + 1, :], (CAP, tok)) == slot_no).astype(F32) for e in range(2 * EB)], axis=0)
        oht[2 * b] = hot[0:EB * CAP].astype(BF)
        oht[2 * b + 1] = hot[EB * CAP:].astype(BF)
        oh[b] = jnp.transpose(hot).astype(BF)
        return carry

    lax.fori_loop(0, NB // 2, build, 0)
    macc[...] = jnp.zeros_like(macc)

    total = sq_snd[...]
    for d in range(1, 4):
        sq_copy(d).wait_recv()
    for d in range(1, 4):
        total = total + sq_recv[d - 1]
    inv_rows = lax.rsqrt(total / model_width + EPS)
    inv = jnp.transpose(jnp.broadcast_to(inv_rows[0:1, :], (tok, tok)))[:, 0:1]
    bnorm[...] = (h_ref[...].astype(F32) * inv * pre_ref[...].astype(F32).reshape(1, -1)).astype(BF)

    lbuf[...] = jnp.dot(bnorm[...], wr_ref[...], preferred_element_type=F32)
    htok = tok // 2
    mine = pl.ds(pl.multiple_of(core * htok, htok), htok)

    def logit_pair():
        return remote(lbuf, lrecv1, l_s.at[0], l_r.at[0], emb=partner)

    def logit_across():
        return remote(lsnd2, lrecv2, l_s.at[1], l_r.at[1], emb=across)

    def prob_pair():
        return remote(pbuf.at[mine], pbuf.at[mine], l_s.at[2], l_r.at[2], emb=partner)

    logit_pair().start()

    own_rows = pl.ds(pl.multiple_of(core * half + row * quarter, quarter), quarter)
    other_rows = pl.ds(pl.multiple_of(core * half + (1 - row) * quarter, quarter), quarter)
    pair_rows = pl.ds(pl.multiple_of((1 - core) * half, half), half)

    every = slice(None)

    def z_pair(j, r):
        return remote(zsend.at[j, pair_rows], recv1.at[j], snd_sem.at[0], r, emb=partner)

    def z_across(j, r):
        return remote(snd2.at[j], recv2.at[j], snd_sem.at[1], r, emb=across)

    def g_across(j, r):
        return remote(gall.at[j, own_rows], gall.at[j, own_rows], snd_sem.at[2], r, emb=across)

    def g_pair(j, r):
        return remote(gall.at[j, own_rows], gall.at[j, own_rows], snd_sem.at[3], r, emb=partner)

    def g_forward(j, r):
        return remote(gall.at[j, other_rows], gall.at[j, other_rows], snd_sem.at[4], r, emb=partner)

    def gather(b):
        xbuf[b % 2] = jnp.dot(oht[b], bnorm[...], preferred_element_type=F32).astype(BF)

    gather(0)

    def stage_b(j):
        z_pair(j, s1_r.at[j]).wait_recv()
        snd2[j] = (zsend[j, other_rows, :].astype(F32)
                   + recv1[j, pl.ds(pl.multiple_of((1 - row) * quarter, quarter), quarter), :].astype(F32)).astype(BF)
        z_across(j, s2_r.at[j]).start()
        own2[j] = (zsend[j, own_rows, :].astype(F32)
                   + recv1[j, pl.ds(pl.multiple_of(row * quarter, quarter), quarter), :].astype(F32))

    def stage_c(k):
        z_across(k, s2_r.at[k]).wait_recv()
        z = (own2[k] + recv2[k].astype(F32)).astype(BF).astype(F32)
        low = jax.nn.gelu(z[:, 0:128], approximate=True) * z[:, 128:256]
        mixed = z[:, 256:384]
        high = jax.nn.gelu(mixed, approximate=True) * pltpu.roll(mixed, 64, 1)
        gall[k, own_rows, 0:128] = low.astype(BF)
        gall[k, own_rows, 128:256] = high.astype(BF)
        g_across(k, gy_r.at[k]).start()
        g_pair(k, gp_r.at[k]).start()

    def stage_d(k):
        g_across(k, gy_r.at[k]).wait_recv()
        g_forward(k, gf_r.at[k]).start()

    def step(i, carry):
        slot = i % RING
        for c in ring_copies(i):
            c.wait()
        for e in range(EB):
            z = lax.dot_general(xbuf[i % 2, e * CAP:(e + 1) * CAP, :], ring[slot, e], (((1,), (1,)), ((), ())),
                                preferred_element_type=F32)
            zsend[i, e * CAP:(e + 1) * CAP, :] = z.astype(BF)
        gather(jnp.minimum(i + 1, NB - 1))
        z_pair(i, s1_r.at[i]).start()

        @pl.when(i + RING < NB)
        def _():
            for c in ring_copies(i + RING):
                c.start()

        @pl.when((i % 2 == 0) & (i // 2 + EARLY < NB // 2))
        def _():
            w2_copy(i // 2 + EARLY).start()

        @pl.when(i >= 1)
        def _():
            stage_b(i - 1)

        @pl.when(i >= LAG_C)
        def _():
            stage_c(i - LAG_C)

        @pl.when(i >= LAG_D)
        def _():
            stage_d(i - LAG_D)

        @pl.when(i == 2)
        def _():
            logit_pair().wait_recv()
            lsnd2[...] = lbuf[mine, :] + lrecv1[mine, :]
            logit_across().start()

        @pl.when(i == 5)
        def _():
            logit_across().wait_recv()
            logits = lsnd2[...] + lrecv2[...]
            pbuf[mine, :] = jax.nn.softmax(logits, axis=1)
            prob_pair().start()

        @pl.when(i == 8)
        def _():
            prob_pair().wait_recv()
            pt_ref[...] = jnp.transpose(pbuf[...])
        return carry

    lax.fori_loop(0, NB, step, 0)

    hw = width // 2
    both, first, second = slice(0, width), slice(0, hw), slice(hw, width)

    def combine(p, cols):
        macc[:, cols] += jnp.dot(oh[p], ubuf[p % 2, :, cols], preferred_element_type=F32)

    def arrived(p):
        w2_copy(p).wait()
        for b in (2 * p, 2 * p + 1):
            g_pair(b, gp_r.at[b]).wait_recv()
            g_forward(b, gf_r.at[b]).wait_recv()

    def down(p, cols):
        for e in range(2 * EB):
            b, rows = 2 * p + e // EB, slice(e % EB * CAP, (e % EB + 1) * CAP)
            probs = pt_ref[2 * p * EB + e:2 * p * EB + e + 1, :]
            gate = jnp.sum(oht[b, rows, :].astype(F32) * probs, axis=1, keepdims=True)
            y = jnp.dot(gall[b, rows, 0:192], w2buf[2 * p * EB + e, :, cols], preferred_element_type=F32)
            ubuf[p % 2, e * CAP:(e + 1) * CAP, cols] = (y.astype(BF).astype(F32) * gate).astype(BF)

    def down_both(p):
        arrived(p)
        if p:
            combine(p - 1, both)
        down(p, both)

    down_both(0)
    stage_b(NB - 1)
    stage_c(NB - 3)
    stage_d(NB - 6)
    down_both(1)
    stage_c(NB - 2)
    stage_d(NB - 5)
    down_both(2)
    stage_d(NB - 4)
    down_both(3)
    stage_c(NB - 1)
    stage_d(NB - 3)
    down_both(4)
    stage_d(NB - 2)
    down_both(5)
    stage_d(NB - 1)
    down_both(6)

    part = tok // 4

    def rs_copy(d, col):
        peer = (ffn + d) % 4
        cols = pl.ds(col * hw, hw)
        return remote(macc.at[pl.ds(pl.multiple_of(peer * part, part), part), cols], mrecv.at[d - 1, :, cols],
                      rs_s.at[d - 1, col], rs_r.at[d - 1, col], ffn=peer)

    arrived(7)
    combine(6, both)
    down(7, first)
    combine(7, first)
    for d in (2, 1, 3):
        rs_copy(d, 0).start()
    down(7, second)
    combine(7, second)
    for d in (2, 1, 3):
        rs_copy(d, 1).start()

    my_tok = pl.ds(pl.multiple_of(ffn * part, part), part)
    for c in (z_pair, z_across, g_across, g_pair, g_forward):
        c(every, s1_r.at[0]).wait_send()
    logit_pair().wait_send()
    logit_across().wait_send()
    prob_pair().wait_send()
    m = macc[my_tok, :]
    for d in range(1, 4):
        sq_copy(d).wait_send()
        rs_copy(d, 0).wait_recv()
        rs_copy(d, 1).wait_recv()
    for d in range(1, 4):
        m = m + mrecv[d - 1]
    mown[...] = m
    m2 = m * m
    tq_snd[...] = m2[:, 0:128] + m2[:, 128:256] + m2[:, 256:384] + m2[:, 384:512]

    def tq_copy(d):
        return remote(tq_snd, tq_recv.at[d - 1], tq_s.at[d - 1], tq_r.at[d - 1], emb=(emb + d) % 4)

    for d in (2, 3, 1):
        tq_copy(d).start()
    for d in range(1, 4):
        rs_copy(d, 0).wait_send()
        rs_copy(d, 1).wait_send()
        tq_copy(d).wait_recv()
    tot = tq_snd[...]
    for d in range(1, 4):
        tot = tot + tq_recv[d - 1]
    inv_post = lax.rsqrt(jnp.sum(tot, axis=1, keepdims=True) / model_width + EPS)
    res = h_ref[my_tok, :].astype(F32) + mown[...] * inv_post * post_ref[...].astype(F32).reshape(1, -1)
    obuf[...] = res.astype(BF)

    def ag_copy(d):
        return remote(obuf, o_ref.at[my_tok], ag_s.at[d - 1], ag_r.at[d - 1], ffn=(ffn + d) % 4)

    for d in (2, 1, 3):
        ag_copy(d).start()
    keep = pltpu.make_async_copy(obuf, o_ref.at[my_tok], in_sem.at[0])
    keep.start()
    for d in range(1, 4):
        tq_copy(d).wait_send()
        ag_copy(d).wait_recv()
    keep.wait()
    for d in range(1, 4):
        ag_copy(d).wait_send()


def solution(mesh):
    emb_size = mesh.shape['emb']

    def local_block(hidden, norm_pre, norm_post, w_router, w_gate, w_up, w_down, choice):
        tok, width = hidden.shape
        experts, _, fw = w_gate.shape
        dma = pltpu.SemaphoreType.DMA
        vm = pltpu.VMEM
        rows = EB * CAP
        return pl.pallas_call(
            functools.partial(kernel, width * emb_size),
            out_shape=jax.ShapeDtypeStruct((tok, width), BF),
            in_specs=[pl.BlockSpec(memory_space=pl.ANY)] * 8,
            out_specs=pl.BlockSpec(memory_space=pl.ANY),
            scratch_shapes=[
                vm((tok, width), BF), vm((width,), BF), vm((width,), BF), vm((width, experts), BF), vm((8, tok), jnp.int32),
                vm((RING, EB, 2 * fw, width), BF), vm((experts, fw, width), BF),
                vm((NB, rows, tok), BF), vm((NB // 2, tok, 2 * rows), BF), vm((tok, width), BF),
                vm((NB, rows, 2 * fw), BF), vm((NB, rows // 2, 2 * fw), BF),
                vm((NB, rows // 4, 2 * fw), BF), vm((NB, rows // 4, 2 * fw), BF), vm((NB, rows // 4, 2 * fw), F32),
                vm((NB, rows, 256), BF), vm((experts, tok), F32), vm((experts, tok), F32),
                vm((tok, experts), F32), vm((tok, experts), F32), vm((tok // 2, experts), F32),
                vm((tok // 2, experts), F32), vm((tok, experts), F32),
                vm((8, tok), F32), vm((3, 8, tok), F32),
                vm((tok, width), F32), vm((2, 2 * rows, width), BF), vm((3, tok // 4, width), F32), vm((tok // 4, width), F32),
                vm((tok // 4, 128), F32), vm((3, tok // 4, 128), F32), vm((tok // 4, width), BF), vm((2, rows, width), BF),
                dma((5,)), dma((RING, 4)), dma((NB // 2,)),
                dma((5,)), dma((NB,)), dma((NB,)), dma((NB,)), dma((NB,)), dma((NB,)),
                dma((3,)), dma((3,)), dma((3,)), dma((3,)), dma((3, 2)), dma((3, 2)), dma((3,)), dma((3,)), dma((3,)), dma((3,)),
            ],
            compiler_params=pltpu.CompilerParams(
                collective_id=0, has_side_effects=True, vmem_limit_bytes=67043328),
        )(hidden, norm_pre, norm_post, w_router, choice.T,
          jnp.swapaxes(w_gate, 1, 2), jnp.swapaxes(w_up, 1, 2), w_down)

    in_specs = (P('dp', 'emb'), P('emb'), P('emb'), P('emb', None), P(None, 'emb', 'ffn'), P(None, 'emb', 'ffn'), P(None, 'ffn', 'emb'), P('dp', None))
    return jax.shard_map(local_block, mesh=mesh, in_specs=in_specs, out_specs=P('dp', 'emb'), check_vma=False)
```

```python
import functools

import jax
import jax.numpy as jnp
from jax import lax
from jax.experimental import pallas as pl
from jax.experimental.pallas import tpu as pltpu
from jax.sharding import PartitionSpec as P

EPS = 1e-5
MESH = pl.DeviceIdType.MESH
BF = jnp.bfloat16
F32 = jnp.float32
EB = 8
CAP = 16
NK = 8
NB = 16
QUART = 48


def remote(src, dst, send, recv, **where):
    return pltpu.make_async_remote_copy(
        src_ref=src, dst_ref=dst, send_sem=send, recv_sem=recv,
        device_id=where, device_id_type=MESH)


def kernel(model_width, h_hbm, pre_hbm, post_hbm, wr_hbm, choice_hbm, w0_ref, w1_ref, w2_ref, o_ref,
           h_ref, pre_ref, post_ref, wr_ref, choice_ref, hx_ref, cx_ref,
           w01, w2buf, oht, ohx, oh, bnorm, bother, zsend, recv1, snd2, recv2, own2, gall, gx, pos_ref, posx_ref, pt_ref,
           lbuf, lrecv1, lsnd2, lrecv2, pbuf, sq_snd, sq_recv, macc, ubuf, mrecv, mown, tq_snd, tq_recv, obuf, xbuf,
           in_sem, w01_sem, w2_sem, snd_sem, s1_r, s2_r, gy_r, gp_r, gf_r, hs_r, ha_r, f1_r, f2_r,
           l_s, l_r, x_s, x_r, sq_s, sq_r, rs_s, rs_r, tq_s, tq_r, ag_s, ag_r):
    dp = lax.axis_index("dp")
    ffn = lax.axis_index("ffn")
    emb = lax.axis_index("emb")
    xp = 1 - dp
    core = emb % 2
    row = emb // 2
    partner = emb + 1 - 2 * core
    across = (emb + 2) % 4
    tok, width = h_ref.shape
    half = EB * CAP // 2
    quarter = half // 2

    barrier = pltpu.get_barrier_semaphore()
    for d in range(1, 4):
        pl.semaphore_signal(barrier, inc=1, device_id={"ffn": (ffn + d) % 4}, device_id_type=MESH)
        pl.semaphore_signal(barrier, inc=1, device_id={"emb": (emb + d) % 4}, device_id_type=MESH)
    for d in range(4):
        pl.semaphore_signal(barrier, inc=1, device_id={"dp": xp, "emb": (emb + d) % 4}, device_id_type=MESH)

    loads = [pltpu.make_async_copy(a, b, in_sem.at[n]) for n, (a, b) in enumerate(
        [(h_hbm, h_ref), (choice_hbm, choice_ref), (pre_hbm, pre_ref), (wr_hbm, wr_ref), (post_hbm, post_ref)])]
    for c in loads:
        c.start()

    def w01_copies(k):
        e0 = pl.ds((dp * NK + k) * EB, EB)
        return [
            pltpu.make_async_copy(w0_ref.at[e0, pl.ds(0, 128)], w01.at[k, :, pl.ds(0, 128)], w01_sem.at[k, 0]),
            pltpu.make_async_copy(w1_ref.at[e0, pl.ds(0, 128)], w01.at[k, :, pl.ds(128, 128)], w01_sem.at[k, 1]),
            pltpu.make_async_copy(w0_ref.at[e0, pl.ds(128, 64)], w01.at[k, :, pl.ds(256, 64)], w01_sem.at[k, 2]),
            pltpu.make_async_copy(w1_ref.at[e0, pl.ds(128, 64)], w01.at[k, :, pl.ds(320, 64)], w01_sem.at[k, 3]),
        ]

    def pair_no(n):
        return (dp if n % 2 == 0 else xp) * (NK // 2) + n // 2

    def w2_copy(n):
        e0 = pl.ds(pair_no(n) * 2 * EB, 2 * EB)
        return pltpu.make_async_copy(w2_ref.at[e0], w2buf.at[e0], w2_sem.at[n])

    for c in loads:
        c.wait()
    for k in range(NK):
        for c in w01_copies(k):
            c.start()

    hf = h_ref[...].astype(F32)
    sq = jnp.sum(hf * hf, axis=1, keepdims=True)
    sq_snd[...] = jnp.transpose(jnp.broadcast_to(sq, (tok, tok)))[0:8]

    pl.semaphore_wait(barrier, 10)

    def sq_copy(n):
        where = dict(emb=(emb + n + 1) % 4) if n < 3 else dict(dp=xp, emb=(emb + n - 3) % 4)
        return remote(sq_snd, sq_recv.at[n], sq_s.at[n], sq_r.at[n], **where)

    def h_copy():
        return remote(h_ref, hx_ref, x_s.at[0], x_r.at[0], dp=xp)

    def c_copy():
        return remote(choice_ref, cx_ref, x_s.at[1], x_r.at[1], dp=xp)

    for n in range(7):
        sq_copy(n).start()
    c_copy().start()
    h_copy().start()

    experts = lax.broadcasted_iota(jnp.int32, (tok, tok), 0)
    lanes = lax.broadcasted_iota(jnp.int32, (tok, tok), 1)
    upper = (experts < lanes).astype(F32).astype(BF)
    slot_no = lax.broadcasted_iota(jnp.int32, (CAP, tok), 0).astype(F32)

    def slots(choices, out):
        assigned = jnp.zeros((tok, tok), F32)
        for k in range(choices.shape[0]):
            assigned = assigned + (jnp.broadcast_to(choices[k:k + 1, :], (tok, tok)) == experts).astype(F32)
        before = jnp.dot(assigned.astype(BF), upper, preferred_element_type=F32)
        out[...] = jnp.where(assigned > 0.5, before, 1000.0)

    def hot_rows(rows):
        return jnp.concatenate(
            [(jnp.broadcast_to(rows[e:e + 1, :], (CAP, tok)) == slot_no).astype(F32) for e in range(2 * EB)], axis=0)

    slots(choice_ref, pos_ref)

    def build(b, carry):
        hot = hot_rows(pos_ref[pl.ds(pl.multiple_of(b * 2 * EB, 2 * EB), 2 * EB), :])
        oht[b] = hot.astype(BF)
        oh[b] = jnp.transpose(hot).astype(BF)
        return carry

    lax.fori_loop(0, NB // 2, build, 0)
    macc[...] = jnp.zeros_like(macc)

    def normed(x, total):
        inv_rows = lax.rsqrt(total / model_width + EPS)
        inv = jnp.transpose(jnp.broadcast_to(inv_rows[0:1, :], (tok, tok)))[:, 0:1]
        return (x[...].astype(F32) * inv * pre_ref[...].astype(F32).reshape(1, -1)).astype(BF)

    for n in range(3):
        sq_copy(n).wait_recv()
    bnorm[...] = normed(h_ref, sq_snd[...] + sq_recv[0] + sq_recv[1] + sq_recv[2])

    lbuf[...] = jnp.dot(bnorm[...], wr_ref[...], preferred_element_type=F32)
    htok = tok // 2
    mine = pl.ds(pl.multiple_of(core * htok, htok), htok)

    def logit_pair():
        return remote(lbuf, lrecv1, l_s.at[0], l_r.at[0], emb=partner)

    def logit_across():
        return remote(lsnd2, lrecv2, l_s.at[1], l_r.at[1], emb=across)

    def prob_pair():
        return remote(pbuf.at[mine], pbuf.at[mine], l_s.at[2], l_r.at[2], emb=partner)

    logit_pair().start()

    own_rows = pl.ds(pl.multiple_of(core * half + row * quarter, quarter), quarter)
    other_rows = pl.ds(pl.multiple_of(core * half + (1 - row) * quarter, quarter), quarter)
    pair_rows = pl.ds(pl.multiple_of((1 - core) * half, half), half)
    own_g = pl.ds(pl.multiple_of((core * 2 + row) * QUART, 16), QUART)
    other_g = pl.ds(pl.multiple_of((core * 2 + 1 - row) * QUART, 16), QUART)

    every = slice(None)

    def z_pair(j, r):
        return remote(zsend.at[j, pair_rows], recv1.at[j], snd_sem.at[0], r, emb=partner)

    def z_across(j, r):
        return remote(snd2.at[j], recv2.at[j], snd_sem.at[1], r, emb=across)

    def at_own(k, rows):
        return gall.at[pl.ds(dp * NK, NK) if k is None else dp * NK + k, rows]

    def at_other(k, rows):
        return gall.at[pl.ds(xp * NK, NK) if k is None else xp * NK + k, rows]

    def g_across(k, r):
        return remote(at_own(k, own_g), at_own(k, own_g), snd_sem.at[2], r, emb=across)

    def g_pair(k, r):
        return remote(at_own(k, own_g), at_own(k, own_g), snd_sem.at[3], r, emb=partner)

    def g_forward(k, r):
        return remote(at_own(k, other_g), at_own(k, other_g), snd_sem.at[4], r, emb=partner)

    def x_same(k, r):
        return remote(gx if k is None else gx.at[k], at_own(k, own_g), snd_sem.at[5], r, dp=xp)

    def x_across(k, r):
        return remote(gx if k is None else gx.at[k], at_own(k, own_g), snd_sem.at[6], r, dp=xp, emb=across)

    def x_forward1(k, r):
        return remote(at_other(k, own_g), at_other(k, own_g), snd_sem.at[7], r, emb=partner)

    def x_forward2(k, r):
        return remote(at_other(k, other_g), at_other(k, other_g), snd_sem.at[8], r, emb=partner)

    rows_k = EB * CAP

    def gather_own(k):
        part_k = slice(k % 2 * rows_k, (k % 2 + 1) * rows_k)
        x = jnp.dot(oht[dp * (NK // 2) + k // 2, part_k, :], bnorm[...], preferred_element_type=F32)
        xbuf[k % 2, 0] = x.astype(BF)

    def gather_other(k):
        part_k = slice(k % 2 * rows_k, (k % 2 + 1) * rows_k)
        x = jnp.dot(ohx[k // 2, part_k, :], bother[...], preferred_element_type=F32)
        xbuf[k % 2, 1] = x.astype(BF)

    gather_own(0)

    c_copy().wait_recv()
    slots(cx_ref, posx_ref)

    def buildx(b, carry):
        at = pl.multiple_of(dp * NK * EB + b * 2 * EB, 2 * EB)
        ohx[b] = hot_rows(posx_ref[pl.ds(at, 2 * EB), :]).astype(BF)
        return carry

    lax.fori_loop(0, NK // 2, buildx, 0)
    for n in range(3, 7):
        sq_copy(n).wait_recv()
    h_copy().wait_recv()
    bother[...] = normed(hx_ref, sq_recv[3] + sq_recv[4] + sq_recv[5] + sq_recv[6])
    gather_other(0)

    def products(k):
        for c in w01_copies(k):
            c.wait()
        for e in range(EB):
            rows = slice(e * CAP, (e + 1) * CAP)
            x = jnp.concatenate([xbuf[k % 2, 0, rows, :], xbuf[k % 2, 1, rows, :]], axis=0)
            z = lax.dot_general(x, w01[k, e], (((1,), (1,)), ((), ())), preferred_element_type=F32).astype(BF)
            zsend[2 * k, rows, :] = z[0:CAP]
            zsend[2 * k + 1, rows, :] = z[CAP:]
        if k + 1 < NK:
            gather_own(k + 1)
            gather_other(k + 1)
        for j in (2 * k + 1, 2 * k):
            z_pair(j, s1_r.at[j]).start()

    def chip_sum(j):
        z_pair(j, s1_r.at[j]).wait_recv()
        snd2[j] = (zsend[j, other_rows, :].astype(F32)
                   + recv1[j, pl.ds(pl.multiple_of((1 - row) * quarter, quarter), quarter), :].astype(F32)).astype(BF)
        z_across(j, s2_r.at[j]).start()
        own2[j] = (zsend[j, own_rows, :].astype(F32)
                   + recv1[j, pl.ds(pl.multiple_of(row * quarter, quarter), quarter), :].astype(F32))

    low_lane = lax.broadcasted_iota(jnp.int32, (CAP, 128), 1) < 64

    def activation(j):
        z_across(j, s2_r.at[j]).wait_recv()
        z = (own2[j] + recv2[j].astype(F32)).astype(BF).astype(F32)
        low = (jax.nn.gelu(z[:, 0:128], approximate=True) * z[:, 128:256]).astype(BF)
        mixed = z[:, 256:384]
        high = jax.nn.gelu(mixed, approximate=True) * pltpu.roll(mixed, 64, 1)
        packed = jnp.where(low_lane, high[0:CAP], pltpu.roll(high[CAP:], 64, 1)).astype(BF)
        return jnp.concatenate([low, packed], axis=0)

    def stage_b(k):
        chip_sum(2 * k + 1)
        chip_sum(2 * k)

    def stage_c(k):
        gx[k] = activation(2 * k + 1)
        x_across(k, ha_r.at[k]).start()
        x_same(k, hs_r.at[k]).start()
        gall[dp * NK + k, own_g, :] = activation(2 * k)
        g_across(k, gy_r.at[k]).start()
        g_pair(k, gp_r.at[k]).start()

    def stage_d(k):
        g_across(k, gy_r.at[k]).wait_recv()
        g_forward(k, gf_r.at[k]).start()
        remote(gx.at[k], at_other(k, own_g), snd_sem.at[5], hs_r.at[k], dp=xp).wait_recv()
        x_forward1(k, f1_r.at[k]).start()
        remote(gx.at[k], at_other(k, other_g), snd_sem.at[6], ha_r.at[k], dp=xp, emb=across).wait_recv()
        x_forward2(k, f2_r.at[k]).start()

    hw = width // 2
    both, first, second = slice(0, width), slice(0, hw), slice(hw, width)

    def combine(n, cols):
        macc[:, cols] += jnp.dot(oh[pair_no(n)], ubuf[n % 2, :, cols], preferred_element_type=F32)

    def arrived(n):
        w2_copy(n).wait()
        for k in (n // 2 * 2, n // 2 * 2 + 1):
            if n % 2 == 0:
                g_pair(k, gp_r.at[k]).wait_recv()
                g_forward(k, gf_r.at[k]).wait_recv()
            else:
                x_forward1(k, f1_r.at[k]).wait_recv()
                x_forward2(k, f2_r.at[k]).wait_recv()

    def down(n, cols):
        p = pair_no(n)
        probs = pt_ref[pl.ds(pl.multiple_of(p * 2 * EB, 2 * EB), 2 * EB), :]
        for e in range(2 * EB):
            b, q, w = 2 * p + e // EB, e % EB // 2, e % 2
            gate = jnp.sum(oht[p, e * CAP:(e + 1) * CAP, :].astype(F32) * probs[e:e + 1, :], axis=1, keepdims=True)
            low = gall[b, q * QUART + w * CAP:q * QUART + (w + 1) * CAP, :]
            high = gall[b, q * QUART + 2 * CAP:(q + 1) * QUART, w * 64:(w + 1) * 64]
            y = jnp.dot(jnp.concatenate([low, high], axis=1), w2buf[2 * EB * p + e, :, cols], preferred_element_type=F32)
            ubuf[n % 2, e * CAP:(e + 1) * CAP, cols] = (y.astype(BF).astype(F32) * gate).astype(BF)

    def down_both(n):
        arrived(n)
        if n:
            combine(n - 1, both)
        down(n, both)

    def logits_sum():
        logit_pair().wait_recv()
        lsnd2[...] = lbuf[mine, :] + lrecv1[mine, :]
        logit_across().start()

    def probabilities():
        logit_across().wait_recv()
        logits = lsnd2[...] + lrecv2[...]
        pbuf[mine, :] = jax.nn.softmax(logits, axis=1)
        prob_pair().start()

    def gates():
        prob_pair().wait_recv()
        pt_ref[...] = jnp.transpose(pbuf[...])

    products(0)
    products(1)
    stage_b(0)
    for n in range(4):
        w2_copy(n).start()
    products(2)
    stage_b(1)
    logits_sum()
    for n in range(4, 8):
        w2_copy(n).start()
    products(3)
    stage_b(2)
    stage_c(0)
    products(4)
    stage_b(3)
    stage_c(1)
    probabilities()
    products(5)
    stage_b(4)
    stage_c(2)
    stage_d(0)
    products(6)
    stage_b(5)
    stage_c(3)
    stage_d(1)
    gates()
    products(7)
    stage_b(6)
    stage_c(4)
    stage_d(2)
    down_both(0)
    stage_b(7)
    down_both(1)
    stage_c(5)
    stage_d(3)
    down_both(2)
    stage_c(6)
    stage_d(4)
    down_both(3)
    stage_c(7)
    stage_d(5)
    down_both(4)
    stage_d(6)
    down_both(5)
    stage_d(7)
    down_both(6)

    part = tok // 4

    def rs_copy(d, col):
        peer = (ffn + d) % 4
        cols = pl.ds(col * hw, hw)
        return remote(macc.at[pl.ds(pl.multiple_of(peer * part, part), part), cols], mrecv.at[d - 1, :, cols],
                      rs_s.at[d - 1, col], rs_r.at[d - 1, col], ffn=peer)

    arrived(7)
    combine(6, both)
    down(7, first)
    combine(7, first)
    for d in (2, 1, 3):
        rs_copy(d, 0).start()
    down(7, second)
    combine(7, second)
    for d in (2, 1, 3):
        rs_copy(d, 1).start()

    my_tok = pl.ds(pl.multiple_of(ffn * part, part), part)
    for c in (z_pair, z_across):
        c(every, s1_r.at[0]).wait_send()
    for c in (g_across, g_pair, g_forward, x_same, x_across, x_forward1, x_forward2):
        c(None, gy_r.at[0]).wait_send()
    h_copy().wait_send()
    c_copy().wait_send()
    for n in range(7):
        sq_copy(n).wait_send()
    logit_pair().wait_send()
    logit_across().wait_send()
    prob_pair().wait_send()
    m = macc[my_tok, :]
    for d in range(1, 4):
        rs_copy(d, 0).wait_recv()
        rs_copy(d, 1).wait_recv()
    for d in range(1, 4):
        m = m + mrecv[d - 1]
    mown[...] = m
    m2 = m * m
    tq_snd[...] = m2[:, 0:128] + m2[:, 128:256] + m2[:, 256:384] + m2[:, 384:512]

    def tq_copy(d):
        return remote(tq_snd, tq_recv.at[d - 1], tq_s.at[d - 1], tq_r.at[d - 1], emb=(emb + d) % 4)

    for d in (2, 3, 1):
        tq_copy(d).start()
    for d in range(1, 4):
        rs_copy(d, 0).wait_send()
        rs_copy(d, 1).wait_send()
        tq_copy(d).wait_recv()
    tot = tq_snd[...]
    for d in range(1, 4):
        tot = tot + tq_recv[d - 1]
    inv_post = lax.rsqrt(jnp.sum(tot, axis=1, keepdims=True) / model_width + EPS)
    res = h_ref[my_tok, :].astype(F32) + mown[...] * inv_post * post_ref[...].astype(F32).reshape(1, -1)
    obuf[...] = res.astype(BF)

    def ag_copy(d):
        return remote(obuf, o_ref.at[my_tok], ag_s.at[d - 1], ag_r.at[d - 1], ffn=(ffn + d) % 4)

    for d in (2, 1, 3):
        ag_copy(d).start()
    keep = pltpu.make_async_copy(obuf, o_ref.at[my_tok], in_sem.at[0])
    keep.start()
    for d in range(1, 4):
        tq_copy(d).wait_send()
        ag_copy(d).wait_recv()
    keep.wait()
    for d in range(1, 4):
        ag_copy(d).wait_send()


def solution(mesh):
    emb_size = mesh.shape['emb']

    def local_block(hidden, norm_pre, norm_post, w_router, w_gate, w_up, w_down, choice):
        tok, width = hidden.shape
        experts, _, fw = w_gate.shape
        dma = pltpu.SemaphoreType.DMA
        vm = pltpu.VMEM
        rows = EB * CAP
        return pl.pallas_call(
            functools.partial(kernel, width * emb_size),
            out_shape=jax.ShapeDtypeStruct((tok, width), BF),
            in_specs=[pl.BlockSpec(memory_space=pl.ANY)] * 8,
            out_specs=pl.BlockSpec(memory_space=pl.ANY),
            scratch_shapes=[
                vm((tok, width), BF), vm((width,), BF), vm((width,), BF), vm((width, experts), BF), vm((8, tok), jnp.int32),
                vm((tok, width), BF), vm((8, tok), jnp.int32),
                vm((NK, EB, 2 * fw, width), BF), vm((experts, fw, width), BF),
                vm((NB // 2, 2 * rows, tok), BF), vm((NK // 2, 2 * rows, tok), BF), vm((NB // 2, tok, 2 * rows), BF),
                vm((tok, width), BF), vm((tok, width), BF),
                vm((NB, rows, 2 * fw), BF), vm((NB, rows // 2, 2 * fw), BF),
                vm((NB, rows // 4, 2 * fw), BF), vm((NB, rows // 4, 2 * fw), BF), vm((NB, rows // 4, 2 * fw), F32),
                vm((NB, 4 * QUART, 128), BF), vm((NK, QUART, 128), BF),
                vm((experts, tok), F32), vm((experts, tok), F32), vm((experts, tok), F32),
                vm((tok, experts), F32), vm((tok, experts), F32), vm((tok // 2, experts), F32),
                vm((tok // 2, experts), F32), vm((tok, experts), F32),
                vm((8, tok), F32), vm((7, 8, tok), F32),
                vm((tok, width), F32), vm((2, 2 * rows, width), BF), vm((3, tok // 4, width), F32), vm((tok // 4, width), F32),
                vm((tok // 4, 128), F32), vm((3, tok // 4, 128), F32), vm((tok // 4, width), BF), vm((2, 2, rows, width), BF),
                dma((5,)), dma((NK, 4)), dma((NB // 2,)),
                dma((9,)), dma((NB,)), dma((NB,)), dma((NK,)), dma((NK,)), dma((NK,)), dma((NK,)), dma((NK,)), dma((NK,)), dma((NK,)),
                dma((3,)), dma((3,)), dma((2,)), dma((2,)), dma((7,)), dma((7,)),
                dma((3, 2)), dma((3, 2)), dma((3,)), dma((3,)), dma((3,)), dma((3,)),
            ],
            compiler_params=pltpu.CompilerParams(
                collective_id=0, has_side_effects=True, vmem_limit_bytes=67043328),
        )(hidden, norm_pre, norm_post, w_router, choice.T,
          jnp.swapaxes(w_gate, 1, 2), jnp.swapaxes(w_up, 1, 2), w_down)

    in_specs = (P('dp', 'emb'), P('emb'), P('emb'), P('emb', None), P(None, 'emb', 'ffn'), P(None, 'emb', 'ffn'), P(None, 'ffn', 'emb'), P('dp', None))
    return jax.shard_map(local_block, mesh=mesh, in_specs=in_specs, out_specs=P('dp', 'emb'), check_vma=False)
```

```python
import functools

import jax
import jax.numpy as jnp
from jax import lax
from jax.experimental import pallas as pl
from jax.experimental.pallas import tpu as pltpu
from jax.sharding import PartitionSpec as P

EPS = 1e-5
MESH = pl.DeviceIdType.MESH
BF = jnp.bfloat16
F32 = jnp.float32
EB = 8
CAP = 16
NK = 8
NB = 16
DIRECT = 7
QUART = 48


def remote(src, dst, send, recv, **where):
    return pltpu.make_async_remote_copy(
        src_ref=src, dst_ref=dst, send_sem=send, recv_sem=recv,
        device_id=where, device_id_type=MESH)


def kernel(model_width, h_hbm, pre_hbm, post_hbm, wr_hbm, choice_hbm, w0_ref, w1_ref, w2_ref, o_ref,
           h_ref, pre_ref, post_ref, wr_ref, choice_ref, hx_ref, cx_ref,
           w01, w2buf, oht, ohx, oh, bnorm, bother, zsend, recv1, snd2, recv2, own2, gall, gx, pos_ref, posx_ref, pt_ref,
           lbuf, lrecv1, lsnd2, lrecv2, pbuf, sq_snd, sq_recv, macc, ubuf, mrecv, mown, tq_snd, tq_recv, obuf, xbuf,
           in_sem, w_sem, snd_sem, s1_r, s2_r, gy_r, hs_r, ha_r, ga_r,
           l_s, l_r, x_s, x_r, sq_s, sq_r, rs_s, rs_r, tq_s, tq_r, ag_s, ag_r):
    dp = lax.axis_index("dp")
    ffn = lax.axis_index("ffn")
    emb = lax.axis_index("emb")
    xp = 1 - dp
    core = emb % 2
    row = emb // 2
    partner = emb + 1 - 2 * core
    across = (emb + 2) % 4
    tok, width = h_ref.shape
    half = EB * CAP // 2
    quarter = half // 2

    barrier = pltpu.get_barrier_semaphore()
    for d in range(1, 4):
        pl.semaphore_signal(barrier, inc=1, device_id={"ffn": (ffn + d) % 4}, device_id_type=MESH)
        pl.semaphore_signal(barrier, inc=1, device_id={"emb": (emb + d) % 4}, device_id_type=MESH)
    for d in range(4):
        pl.semaphore_signal(barrier, inc=1, device_id={"dp": xp, "emb": (emb + d) % 4}, device_id_type=MESH)

    loads = [pltpu.make_async_copy(a, b, in_sem.at[n]) for n, (a, b) in enumerate(
        [(h_hbm, h_ref), (choice_hbm, choice_ref), (pre_hbm, pre_ref), (wr_hbm, wr_ref), (post_hbm, post_ref)])]
    for c in loads:
        c.start()

    def w01_start(k):
        e0 = pl.ds((dp * NK + k) * EB, EB)
        pltpu.make_async_copy(w0_ref.at[e0, pl.ds(0, 128)], w01.at[k, :, pl.ds(0, 128)], w_sem.at[k]).start()
        pltpu.make_async_copy(w1_ref.at[e0, pl.ds(0, 128)], w01.at[k, :, pl.ds(128, 128)], w_sem.at[k]).start()
        pltpu.make_async_copy(w0_ref.at[e0, pl.ds(128, 64)], w01.at[k, :, pl.ds(256, 64)], w_sem.at[k]).start()
        pltpu.make_async_copy(w1_ref.at[e0, pl.ds(128, 64)], w01.at[k, :, pl.ds(320, 64)], w_sem.at[k]).start()

    def w01_wait(k):
        pltpu.make_async_copy(w01.at[k], w01.at[k], w_sem.at[k]).wait()

    def pair_no(n):
        return (dp if n % 2 == 0 else xp) * (NK // 2) + n // 2

    def w2_copy(n):
        e0 = pl.ds(pair_no(n) * 2 * EB, 2 * EB)
        return pltpu.make_async_copy(w2_ref.at[e0], w2buf.at[e0], w_sem.at[n])

    for c in loads:
        c.wait()
    hf = h_ref[...].astype(F32)
    sq = jnp.sum(hf * hf, axis=1, keepdims=True)
    sq_snd[...] = jnp.transpose(jnp.broadcast_to(sq, (tok, tok)))[0:8]

    pl.semaphore_wait(barrier, 10)

    def sq_copy(n):
        where = dict(emb=(emb + n + 1) % 4) if n < 3 else dict(dp=xp, emb=(emb + n - 3) % 4)
        return remote(sq_snd, sq_recv.at[n], sq_s.at[0], sq_r.at[0 if n < 3 else 1], **where)

    def h_copy():
        return remote(h_ref, hx_ref, x_s.at[0], x_r.at[0], dp=xp)

    def c_copy():
        return remote(choice_ref, cx_ref, x_s.at[1], x_r.at[1], dp=xp)

    for n in range(7):
        sq_copy(n).start()
    c_copy().start()
    h_copy().start()
    for k in range(NK):
        w01_start(k)

    experts = lax.broadcasted_iota(jnp.int32, (tok, tok), 0)
    lanes = lax.broadcasted_iota(jnp.int32, (tok, tok), 1)
    upper = (experts < lanes).astype(F32).astype(BF)
    slot_no = lax.broadcasted_iota(jnp.int32, (CAP, tok), 0).astype(F32)

    def slots(choices, out):
        assigned = jnp.zeros((tok, tok), F32)
        for k in range(choices.shape[0]):
            assigned = assigned + (jnp.broadcast_to(choices[k:k + 1, :], (tok, tok)) == experts).astype(F32)
        before = jnp.dot(assigned.astype(BF), upper, preferred_element_type=F32)
        out[...] = jnp.where(assigned > 0.5, before, 1000.0)

    def hot_rows(rows):
        return jnp.concatenate(
            [(jnp.broadcast_to(rows[e:e + 1, :], (CAP, tok)) == slot_no).astype(F32) for e in range(2 * EB)], axis=0)

    slots(choice_ref, pos_ref)

    def build(b, carry):
        hot = hot_rows(pos_ref[pl.ds(pl.multiple_of(b * 2 * EB, 2 * EB), 2 * EB), :])
        oht[b] = hot.astype(BF)
        oh[b] = jnp.transpose(hot).astype(BF)
        return carry

    lax.fori_loop(0, NB // 2, build, 0)
    macc[...] = jnp.zeros_like(macc)

    def normed(x, total):
        inv_rows = lax.rsqrt(total / model_width + EPS)
        inv = jnp.transpose(jnp.broadcast_to(inv_rows[0:1, :], (tok, tok)))[:, 0:1]
        return (x[...].astype(F32) * inv * pre_ref[...].astype(F32).reshape(1, -1)).astype(BF)

    remote(sq_snd, sq_recv.at[pl.ds(0, 3)], sq_s.at[0], sq_r.at[0], emb=across).wait_recv()
    bnorm[...] = normed(h_ref, sq_snd[...] + sq_recv[0] + sq_recv[1] + sq_recv[2])

    lbuf[...] = jnp.dot(bnorm[...], wr_ref[...], preferred_element_type=F32)
    htok = tok // 2
    mine = pl.ds(pl.multiple_of(core * htok, htok), htok)

    def logit_pair():
        return remote(lbuf, lrecv1, l_s.at[0], l_r.at[0], emb=partner)

    def logit_across():
        return remote(lsnd2, lrecv2, l_s.at[1], l_r.at[1], emb=across)

    def prob_pair():
        return remote(pbuf.at[mine], pbuf.at[mine], l_s.at[2], l_r.at[2], emb=partner)

    logit_pair().start()

    own_rows = pl.ds(pl.multiple_of(core * half + row * quarter, quarter), quarter)
    other_rows = pl.ds(pl.multiple_of(core * half + (1 - row) * quarter, quarter), quarter)
    pair_rows = pl.ds(pl.multiple_of((1 - core) * half, half), half)
    own_g = pl.ds(pl.multiple_of((core * 2 + row) * QUART, 16), QUART)
    other_g = pl.ds(pl.multiple_of((core * 2 + 1 - row) * QUART, 16), QUART)

    every = slice(None)

    def z_pair(k, r):
        return remote(zsend.at[k, :, pair_rows], recv1.at[k], snd_sem.at[0], r, emb=partner)

    def z_across(k, r):
        return remote(snd2.at[k], recv2.at[k], snd_sem.at[1], r, emb=across)

    def g_at(x, k, rows, count=None):
        return gall.at[x * NK + k if count is None else pl.ds(x * NK + k, count), rows]

    def g_copy(sem, r, x, rows, k, count=None, **where):
        return remote(g_at(x, k, rows, count), g_at(x, k, rows, count), snd_sem.at[sem], r, **where)

    def x_copy(sem, r, k, count=None, **where):
        return remote(gx.at[k if count is None else pl.ds(k, count)], g_at(dp, k, own_g, count), snd_sem.at[sem], r, dp=xp, **where)

    theirs = pl.ds(pl.multiple_of((1 - core) * 2 * QUART, 16), 2 * QUART)
    corner = 3 - emb

    rows_k = EB * CAP

    def gather_own(k):
        part_k = slice(k % 2 * rows_k, (k % 2 + 1) * rows_k)
        x = jnp.dot(oht[dp * (NK // 2) + k // 2, part_k, :], bnorm[...], preferred_element_type=F32)
        xbuf[k % 2, 0] = x.astype(BF)

    def gather_other(k):
        part_k = slice(k % 2 * rows_k, (k % 2 + 1) * rows_k)
        x = jnp.dot(ohx[k // 2, part_k, :], bother[...], preferred_element_type=F32)
        xbuf[k % 2, 1] = x.astype(BF)

    gather_own(0)

    c_copy().wait_recv()
    slots(cx_ref, posx_ref)

    def buildx(b, carry):
        at = pl.multiple_of(dp * NK * EB + b * 2 * EB, 2 * EB)
        ohx[b] = hot_rows(posx_ref[pl.ds(at, 2 * EB), :]).astype(BF)
        return carry

    lax.fori_loop(0, NK // 2, buildx, 0)
    remote(sq_snd, sq_recv.at[pl.ds(3, 4)], sq_s.at[0], sq_r.at[1], dp=xp).wait_recv()
    h_copy().wait_recv()
    bother[...] = normed(hx_ref, sq_recv[3] + sq_recv[4] + sq_recv[5] + sq_recv[6])
    gather_other(0)

    def products(k):
        w01_wait(k)
        for e in range(EB):
            rows = slice(e * CAP, (e + 1) * CAP)
            x = jnp.concatenate([xbuf[k % 2, 0, rows, :], xbuf[k % 2, 1, rows, :]], axis=0)
            z = lax.dot_general(x, w01[k, e], (((1,), (1,)), ((), ())), preferred_element_type=F32).astype(BF)
            zsend[k, 0, rows, :] = z[0:CAP]
            zsend[k, 1, rows, :] = z[CAP:]
        if k + 1 < NK:
            gather_own(k + 1)
            gather_other(k + 1)
        z_pair(k, s1_r.at[k]).start()
        w2_copy(k).start()

    def stage_b(k):
        z_pair(k, s1_r.at[k]).wait_recv()
        near = pl.ds(pl.multiple_of(row * quarter, quarter), quarter)
        far = pl.ds(pl.multiple_of((1 - row) * quarter, quarter), quarter)
        snd2[k] = (zsend[k, :, other_rows, :].astype(F32) + recv1[k, :, far, :].astype(F32)).astype(BF)
        z_across(k, s2_r.at[k]).start()
        own2[k] = zsend[k, :, own_rows, :].astype(F32) + recv1[k, :, near, :].astype(F32)

    low_lane = lax.broadcasted_iota(jnp.int32, (CAP, 128), 1) < 64

    def activation(k, g):
        z = (own2[k, g] + recv2[k, g].astype(F32)).astype(BF).astype(F32)
        low = (jax.nn.gelu(z[:, 0:128], approximate=True) * z[:, 128:256]).astype(BF)
        mixed = z[:, 256:384]
        high = jax.nn.gelu(mixed, approximate=True) * pltpu.roll(mixed, 64, 1)
        packed = jnp.where(low_lane, high[0:CAP], pltpu.roll(high[CAP:], 64, 1)).astype(BF)
        return jnp.concatenate([low, packed], axis=0)

    def stage_c(k):
        n = k // 2 * 2
        z_across(k, s2_r.at[k]).wait_recv()
        gx[k] = activation(k, 1)
        x_copy(6, ha_r.at[k], k, emb=across).start()
        x_copy(5, hs_r.at[k], k).start()
        if k >= DIRECT:
            x_copy(9, ga_r.at[n + 1], k, emb=corner).start()
            x_copy(10, ga_r.at[n + 1], k, emb=partner).start()
        gall[dp * NK + k, own_g, :] = activation(k, 0)
        g_copy(2, gy_r.at[k], dp, own_g, k, emb=across).start()
        g_copy(3, ga_r.at[n], dp, own_g, k, emb=partner).start()
        if k >= DIRECT:
            g_copy(11, ga_r.at[n], dp, own_g, k, emb=corner).start()

    def from_across(k):
        return g_copy(2, gy_r.at[k], dp, other_g, k, emb=across)

    def from_x(k, rows, r):
        return g_copy(5, r, xp, rows, k, dp=xp)

    def stage_d(k):
        n = k // 2 * 2
        from_across(k).wait_recv()
        g_copy(4, ga_r.at[n], dp, other_g, k, emb=partner).start()
        from_x(k, own_g, hs_r.at[k]).wait_recv()
        g_copy(7, ga_r.at[n + 1], xp, own_g, k, emb=partner).start()
        from_x(k, other_g, ha_r.at[k]).wait_recv()
        g_copy(8, ga_r.at[n + 1], xp, other_g, k, emb=partner).start()

    hw = width // 2
    both, first, second = slice(0, width), slice(0, hw), slice(hw, width)

    def combine(n, cols):
        macc[:, cols] += jnp.dot(oh[pair_no(n)], ubuf[n % 2, :, cols], preferred_element_type=F32)

    def arrived(n):
        w2_copy(n).wait()
        for k in (n // 2 * 2, n // 2 * 2 + 1):
            if k >= DIRECT and n % 2 == 0:
                from_across(k).wait_recv()
            if k >= DIRECT and n % 2 == 1:
                from_x(k, own_g, hs_r.at[k]).wait_recv()
                from_x(k, other_g, ha_r.at[k]).wait_recv()
        g_copy(3, ga_r.at[n], dp if n % 2 == 0 else xp, theirs, n // 2 * 2, 2, emb=partner).wait_recv()

    def down(n, cols):
        p = pair_no(n)
        probs = pt_ref[pl.ds(pl.multiple_of(p * 2 * EB, 2 * EB), 2 * EB), :]
        for e in range(2 * EB):
            b, q, w = 2 * p + e // EB, e % EB // 2, e % 2
            gate = jnp.sum(oht[p, e * CAP:(e + 1) * CAP, :].astype(F32) * probs[e:e + 1, :], axis=1, keepdims=True)
            low = gall[b, q * QUART + w * CAP:q * QUART + (w + 1) * CAP, :]
            high = gall[b, q * QUART + 2 * CAP:(q + 1) * QUART, w * 64:(w + 1) * 64]
            y = jnp.dot(jnp.concatenate([low, high], axis=1), w2buf[2 * EB * p + e, :, cols], preferred_element_type=F32)
            ubuf[n % 2, e * CAP:(e + 1) * CAP, cols] = (y.astype(BF).astype(F32) * gate).astype(BF)

    def down_both(n):
        arrived(n)
        if n:
            combine(n - 1, both)
        down(n, both)

    def logits_sum():
        logit_pair().wait_recv()
        lsnd2[...] = lbuf[mine, :] + lrecv1[mine, :]
        logit_across().start()

    def probabilities():
        logit_across().wait_recv()
        logits = lsnd2[...] + lrecv2[...]
        pbuf[mine, :] = jax.nn.softmax(logits, axis=1)
        prob_pair().start()

    def gates():
        prob_pair().wait_recv()
        pt_ref[...] = jnp.transpose(pbuf[...])

    products(0)
    products(1)
    stage_b(0)
    products(2)
    stage_b(1)
    logits_sum()
    products(3)
    stage_b(2)
    stage_c(0)
    products(4)
    stage_b(3)
    stage_c(1)
    probabilities()
    products(5)
    stage_b(4)
    stage_c(2)
    stage_d(0)
    products(6)
    stage_b(5)
    stage_c(3)
    stage_d(1)
    gates()
    products(7)
    stage_b(6)
    stage_c(4)
    stage_d(2)
    down_both(0)
    stage_b(7)
    stage_c(5)
    stage_d(3)
    down_both(1)
    stage_d(4)
    stage_c(6)
    down_both(2)
    stage_c(7)
    stage_d(5)
    down_both(3)
    down_both(4)
    stage_d(6)
    down_both(5)
    down_both(6)

    part = tok // 4

    def rs_copy(d, col):
        peer = (ffn + d) % 4
        cols = pl.ds(col * hw, hw)
        return remote(macc.at[pl.ds(pl.multiple_of(peer * part, part), part), cols], mrecv.at[d - 1, :, cols],
                      rs_s.at[0], rs_r.at[col], ffn=peer)

    arrived(7)
    combine(6, both)
    down(7, first)
    combine(7, first)
    for d in (2, 1, 3):
        rs_copy(d, 0).start()
    down(7, second)
    combine(7, second)
    for d in (2, 1, 3):
        rs_copy(d, 1).start()

    my_tok = pl.ds(pl.multiple_of(ffn * part, part), part)
    for c in (z_pair, z_across):
        c(every, s1_r.at[0]).wait_send()
    for sem, x, rows, k, count in ((2, dp, own_g, 0, NK), (3, dp, own_g, 0, NK), (4, dp, other_g, 0, DIRECT),
                                   (7, xp, own_g, 0, DIRECT), (8, xp, other_g, 0, DIRECT), (11, dp, own_g, DIRECT, NK - DIRECT)):
        g_copy(sem, gy_r.at[0], x, rows, k, count, emb=partner).wait_send()
    for sem, k, count in ((5, 0, NK), (6, 0, NK), (9, DIRECT, NK - DIRECT), (10, DIRECT, NK - DIRECT)):
        x_copy(sem, gy_r.at[0], k, count).wait_send()
    h_copy().wait_send()
    c_copy().wait_send()
    remote(sq_recv, sq_recv, sq_s.at[0], sq_r.at[0], dp=xp).wait_send()
    logit_pair().wait_send()
    logit_across().wait_send()
    prob_pair().wait_send()
    m = macc[my_tok, :]
    for col in range(2):
        all_in = mrecv.at[:, :, pl.ds(col * hw, hw)]
        remote(all_in, all_in, rs_s.at[0], rs_r.at[col], ffn=(ffn + 1) % 4).wait_recv()
    for d in range(1, 4):
        m = m + mrecv[d - 1]
    mown[...] = m
    m2 = m * m
    tq_snd[...] = m2[:, 0:128] + m2[:, 128:256] + m2[:, 256:384] + m2[:, 384:512]

    def tq_copy(d):
        return remote(tq_snd, tq_recv.at[d - 1], tq_s.at[0], tq_r.at[0], emb=(emb + d) % 4)

    for d in (2, 3, 1):
        tq_copy(d).start()
    remote(mrecv, mrecv, rs_s.at[0], rs_r.at[0], ffn=(ffn + 1) % 4).wait_send()
    remote(tq_recv, tq_recv, tq_s.at[0], tq_r.at[0], emb=partner).wait()
    tot = tq_snd[...]
    for d in range(1, 4):
        tot = tot + tq_recv[d - 1]
    inv_post = lax.rsqrt(jnp.sum(tot, axis=1, keepdims=True) / model_width + EPS)
    res = h_ref[my_tok, :].astype(F32) + mown[...] * inv_post * post_ref[...].astype(F32).reshape(1, -1)
    obuf[...] = res.astype(BF)

    def ag_copy(d):
        return remote(obuf, o_ref.at[my_tok], ag_s.at[0], ag_r.at[0], ffn=(ffn + d) % 4)

    for d in (2, 1, 3):
        ag_copy(d).start()
    keep = pltpu.make_async_copy(obuf, o_ref.at[my_tok], in_sem.at[0])
    keep.start()
    others = o_ref.at[pl.ds(0, 3 * part)]
    keep.wait()
    remote(others, others, ag_s.at[0], ag_r.at[0], ffn=(ffn + 1) % 4).wait()


def solution(mesh):
    emb_size = mesh.shape['emb']

    def local_block(hidden, norm_pre, norm_post, w_router, w_gate, w_up, w_down, choice):
        tok, width = hidden.shape
        experts, _, fw = w_gate.shape
        dma = pltpu.SemaphoreType.DMA
        vm = pltpu.VMEM
        rows = EB * CAP
        return pl.pallas_call(
            functools.partial(kernel, width * emb_size),
            out_shape=jax.ShapeDtypeStruct((tok, width), BF),
            in_specs=[pl.BlockSpec(memory_space=pl.ANY)] * 8,
            out_specs=pl.BlockSpec(memory_space=pl.ANY),
            scratch_shapes=[
                vm((tok, width), BF), vm((width,), BF), vm((width,), BF), vm((width, experts), BF), vm((8, tok), jnp.int32),
                vm((tok, width), BF), vm((8, tok), jnp.int32),
                vm((NK, EB, 2 * fw, width), BF), vm((experts, fw, width), BF),
                vm((NB // 2, 2 * rows, tok), BF), vm((NK // 2, 2 * rows, tok), BF), vm((NB // 2, tok, 2 * rows), BF),
                vm((tok, width), BF), vm((tok, width), BF),
                vm((NK, 2, rows, 2 * fw), BF), vm((NK, 2, rows // 2, 2 * fw), BF),
                vm((NK, 2, rows // 4, 2 * fw), BF), vm((NK, 2, rows // 4, 2 * fw), BF), vm((NK, 2, rows // 4, 2 * fw), F32),
                vm((NB, 4 * QUART, 128), BF), vm((NK, QUART, 128), BF),
                vm((experts, tok), F32), vm((experts, tok), F32), vm((experts, tok), F32),
                vm((tok, experts), F32), vm((tok, experts), F32), vm((tok // 2, experts), F32),
                vm((tok // 2, experts), F32), vm((tok, experts), F32),
                vm((8, tok), F32), vm((7, 8, tok), F32),
                vm((tok, width), F32), vm((2, 2 * rows, width), BF), vm((3, tok // 4, width), F32), vm((tok // 4, width), F32),
                vm((tok // 4, 128), F32), vm((3, tok // 4, 128), F32), vm((tok // 4, width), BF), vm((2, 2, rows, width), BF),
                dma((5,)), dma((NK,)), dma((12,)), dma((NK,)), dma((NK,)), dma((NK,)), dma((NK,)), dma((NK,)), dma((NK,)),
                dma((3,)), dma((3,)), dma((2,)), dma((2,)), dma((1,)), dma((2,)),
                dma((1,)), dma((2,)), dma((1,)), dma((1,)), dma((1,)), dma((1,)),
            ],
            compiler_params=pltpu.CompilerParams(
                collective_id=0, has_side_effects=True, vmem_limit_bytes=67043328),
        )(hidden, norm_pre, norm_post, w_router, choice.T,
          jnp.swapaxes(w_gate, 1, 2), jnp.swapaxes(w_up, 1, 2), w_down)

    in_specs = (P('dp', 'emb'), P('emb'), P('emb'), P('emb', None), P(None, 'emb', 'ffn'), P(None, 'emb', 'ffn'), P(None, 'ffn', 'emb'), P('dp', None))
    return jax.shard_map(local_block, mesh=mesh, in_specs=in_specs, out_specs=P('dp', 'emb'), check_vma=False)
```

```python
import functools

import jax
import jax.numpy as jnp
from jax import lax
from jax.experimental import pallas as pl
from jax.experimental.pallas import tpu as pltpu
from jax.sharding import PartitionSpec as P

EPS = 1e-5
MESH = pl.DeviceIdType.MESH
BF = jnp.bfloat16
F32 = jnp.float32
LANES = 128
EB = 8
CAP = 16
NK = 8
NB = 16
DIRECT = 7
QUART = 48


def remote(src, dst, send, recv, **where):
    return pltpu.make_async_remote_copy(
        src_ref=src, dst_ref=dst, send_sem=send, recv_sem=recv,
        device_id=where, device_id_type=MESH)


def kernel(model_width, h_hbm, pre_hbm, post_hbm, wr_hbm, choice_hbm, w0_ref, w1_ref, w2_ref, o_ref,
           h_ref, pre_ref, post_ref, wr_ref, choice_ref, hx_ref, cx_ref,
           w01, w2buf, oht, ohx, oh, bnorm, bother, zsend, recv1, snd2, recv2, own2, gall, gx, pos_ref, posx_ref, pt_ref,
           lbuf, lrecv1, lsnd2, lrecv2, pbuf, sq_snd, sq_recv, macc, ubuf, mrecv, mown, tq_snd, tq_recv, obuf, xbuf,
           in_sem, w_sem, snd_sem, s1_r, s2_r, gy_r, hs_r, ha_r, ga_r,
           l_s, l_r, x_s, x_r, sq_s, sq_r, rs_s, rs_r, tq_s, tq_r, ag_s, ag_r):
    dp = lax.axis_index("dp")
    ffn = lax.axis_index("ffn")
    emb = lax.axis_index("emb")
    xp = 1 - dp
    core = emb % 2
    row = emb // 2
    partner = emb + 1 - 2 * core
    across = (emb + 2) % 4
    tok, width = h_ref.shape
    half = EB * CAP // 2
    quarter = half // 2

    barrier = pltpu.get_barrier_semaphore()
    for d in range(1, 4):
        pl.semaphore_signal(barrier, inc=1, device_id={"ffn": (ffn + d) % 4}, device_id_type=MESH)
        pl.semaphore_signal(barrier, inc=1, device_id={"emb": (emb + d) % 4}, device_id_type=MESH)
    for d in range(4):
        pl.semaphore_signal(barrier, inc=1, device_id={"dp": xp, "emb": (emb + d) % 4}, device_id_type=MESH)

    loads = [pltpu.make_async_copy(a, b, in_sem.at[n]) for n, (a, b) in enumerate(
        [(h_hbm, h_ref), (choice_hbm, choice_ref), (pre_hbm, pre_ref), (wr_hbm, wr_ref), (post_hbm, post_ref)])]
    for c in loads:
        c.start()

    def w01_start(k):
        e0 = pl.ds((dp * NK + k) * EB, EB)
        pltpu.make_async_copy(w0_ref.at[e0, pl.ds(0, 128)], w01.at[k, :, pl.ds(0, 128)], w_sem.at[k]).start()
        pltpu.make_async_copy(w1_ref.at[e0, pl.ds(0, 128)], w01.at[k, :, pl.ds(128, 128)], w_sem.at[k]).start()
        pltpu.make_async_copy(w0_ref.at[e0, pl.ds(128, 64)], w01.at[k, :, pl.ds(256, 64)], w_sem.at[k]).start()
        pltpu.make_async_copy(w1_ref.at[e0, pl.ds(128, 64)], w01.at[k, :, pl.ds(320, 64)], w_sem.at[k]).start()

    def w01_wait(k):
        pltpu.make_async_copy(w01.at[k], w01.at[k], w_sem.at[k]).wait()

    def pair_no(n):
        return (dp if n % 2 == 0 else xp) * (NK // 2) + n // 2

    def w2_copy(n):
        e0 = pl.ds(pair_no(n) * 2 * EB, 2 * EB)
        return pltpu.make_async_copy(w2_ref.at[e0], w2buf.at[e0], w_sem.at[n])

    for c in loads:
        c.wait()
    pl.semaphore_wait(barrier, 10)

    def sq_copy(n):
        where = dict(emb=(emb + n + 1) % 4) if n < 3 else dict(dp=xp, emb=(emb + n - 3) % 4)
        return remote(sq_snd, sq_recv.at[n], sq_s, sq_r.at[0 if n < 3 else 1], **where)

    def h_copy():
        return remote(h_ref, hx_ref, x_s.at[0], x_r.at[0], dp=xp)

    def c_copy():
        return remote(choice_ref, cx_ref, x_s.at[1], x_r.at[1], dp=xp)

    c_copy().start()
    h_copy().start()

    hf = h_ref[...].astype(F32)
    sq = jnp.sum(hf * hf, axis=1, keepdims=True)
    sq_snd[...] = jnp.transpose(jnp.broadcast_to(sq, (tok, tok)))[0:8]
    for n in range(7):
        sq_copy(n).start()
    for k in range(NK):
        w01_start(k)

    experts = lax.broadcasted_iota(jnp.int32, (tok, tok), 0)
    lanes = lax.broadcasted_iota(jnp.int32, (tok, tok), 1)
    upper = (experts < lanes).astype(F32).astype(BF)
    slot_no = lax.broadcasted_iota(jnp.int32, (CAP, tok), 0).astype(F32)

    def slots(choices, out):
        assigned = jnp.zeros((tok, tok), F32)
        for k in range(choices.shape[0]):
            assigned = assigned + (jnp.broadcast_to(choices[k:k + 1, :], (tok, tok)) == experts).astype(F32)
        before = jnp.dot(assigned.astype(BF), upper, preferred_element_type=F32)
        out[...] = jnp.where(assigned > 0.5, before, 1000.0)

    def hot_rows(rows):
        return jnp.concatenate(
            [(jnp.broadcast_to(rows[e:e + 1, :], (CAP, tok)) == slot_no).astype(F32) for e in range(2 * EB)], axis=0)

    slots(choice_ref, pos_ref)

    def build(b, carry):
        hot = hot_rows(pos_ref[pl.ds(pl.multiple_of(b * 2 * EB, 2 * EB), 2 * EB), :])
        oht[b] = hot.astype(BF)
        oh[b] = jnp.transpose(hot).astype(BF)
        return carry

    lax.fori_loop(0, NB // 2, build, 0)
    macc[...] = jnp.zeros_like(macc)

    def normed(x, total):
        inv_rows = lax.rsqrt(total / model_width + EPS)
        inv = jnp.transpose(jnp.broadcast_to(inv_rows[0:1, :], (tok, tok)))[:, 0:1]
        return (x[...].astype(F32) * inv * pre_ref[...].astype(F32).reshape(1, -1)).astype(BF)

    remote(sq_snd, sq_recv.at[pl.ds(0, 3)], sq_s, sq_r.at[0], emb=across).wait_recv()
    bnorm[...] = normed(h_ref, functools.reduce(lax.add, [sq_recv[n] for n in range(3)], sq_snd[...]))

    lbuf[...] = jnp.dot(bnorm[...], wr_ref[...], preferred_element_type=F32)
    htok = tok // 2
    mine = pl.ds(pl.multiple_of(core * htok, htok), htok)

    def logit_pair():
        return remote(lbuf, lrecv1, l_s.at[0], l_r.at[0], emb=partner)

    def logit_across():
        return remote(lsnd2, lrecv2, l_s.at[1], l_r.at[1], emb=across)

    def prob_pair():
        return remote(pbuf.at[mine], pbuf.at[mine], l_s.at[2], l_r.at[2], emb=partner)

    logit_pair().start()

    own_rows = pl.ds(pl.multiple_of(core * half + row * quarter, quarter), quarter)
    other_rows = pl.ds(pl.multiple_of(core * half + (1 - row) * quarter, quarter), quarter)
    pair_rows = pl.ds(pl.multiple_of((1 - core) * half, half), half)
    own_g = pl.ds(pl.multiple_of((core * 2 + row) * QUART, 16), QUART)
    other_g = pl.ds(pl.multiple_of((core * 2 + 1 - row) * QUART, 16), QUART)

    every = slice(None)

    def z_pair(k, r, g=every):
        return remote(zsend.at[k, g, pair_rows], recv1.at[k, g], snd_sem.at[0], r, emb=partner)

    def z_across(k, r, g=every):
        return remote(snd2.at[k, g], recv2.at[k, g], snd_sem.at[1], r, emb=across)

    def g_at(x, k, rows, count=None):
        return gall.at[x * NK + k if count is None else pl.ds(x * NK + k, count), rows]

    def g_copy(sem, r, x, rows, k, count=None, **where):
        return remote(g_at(x, k, rows, count), g_at(x, k, rows, count), snd_sem.at[sem], r, **where)

    def x_copy(sem, r, k, count=None, **where):
        return remote(gx.at[k if count is None else pl.ds(k, count)], g_at(dp, k, own_g, count), snd_sem.at[sem], r, dp=xp, **where)

    theirs = pl.ds(pl.multiple_of((1 - core) * 2 * QUART, 16), 2 * QUART)
    corner = 3 - emb

    rows_k = EB * CAP

    def gather_own(k):
        part_k = slice(k % 2 * rows_k, (k % 2 + 1) * rows_k)
        x = jnp.dot(oht[dp * (NK // 2) + k // 2, part_k, :], bnorm[...], preferred_element_type=F32)
        xbuf[k % 2, 0] = x.astype(BF)

    def gather_other(k):
        part_k = slice(k % 2 * rows_k, (k % 2 + 1) * rows_k)
        x = jnp.dot(ohx[k // 2, part_k, :], bother[...], preferred_element_type=F32)
        xbuf[k % 2, 1] = x.astype(BF)

    def products(k, g=every, act=None):
        if act is not None:
            activation_wait(act)
        if g != 1:
            w01_wait(k)
        for e in range(EB):
            rows = slice(e * CAP, (e + 1) * CAP)
            if g == every:
                x = jnp.concatenate([xbuf[k % 2, 0, rows, :], xbuf[k % 2, 1, rows, :]], axis=0)
            else:
                x = xbuf[k % 2, g, rows, :]
            z = lax.dot_general(x, w01[k, e], (((1,), (1,)), ((), ())), preferred_element_type=F32).astype(BF)
            if g != 1:
                zsend[k, 0, rows, :] = z[0:CAP]
            if g != 0:
                zsend[k, 1, rows, :] = z[-CAP:]
        if g != 0 and k + 1 < NK:
            gather_own(k + 1)
            gather_other(k + 1)
        if act is not None:
            activations(act)
        z_pair(k, s1_r.at[NK if g == 1 else k], g).start()
        if act is not None:
            activation_send(act)
        if g != 0:
            w2_copy(k).start()

    def stage_b(k, g=every):
        z_pair(k, s1_r.at[NK if g == 1 else k], g).wait_recv()
        near = pl.ds(pl.multiple_of(row * quarter, quarter), quarter)
        far = pl.ds(pl.multiple_of((1 - row) * quarter, quarter), quarter)
        snd2[k, g] = (zsend[k, g, other_rows, :].astype(F32) + recv1[k, g, far, :].astype(F32)).astype(BF)
        z_across(k, s2_r.at[NK if g == 1 else k], g).start()
        own2[k, g] = zsend[k, g, own_rows, :].astype(F32) + recv1[k, g, near, :].astype(F32)

    low_lane = lax.broadcasted_iota(jnp.int32, (CAP, 128), 1) < 64

    def activation(k, g):
        z = (own2[k, g] + recv2[k, g].astype(F32)).astype(BF).astype(F32)
        low = (jax.nn.gelu(z[:, 0:128], approximate=True) * z[:, 128:256]).astype(BF)
        mixed = z[:, 256:384]
        high = jax.nn.gelu(mixed, approximate=True) * pltpu.roll(mixed, 64, 1)
        packed = jnp.where(low_lane, high[0:CAP], pltpu.roll(high[CAP:], 64, 1)).astype(BF)
        return jnp.concatenate([low, packed], axis=0)

    def activation_wait(k):
        if k == 0:
            z_across(0, s2_r.at[0], 0).wait_recv()
            z_across(0, s2_r.at[NK], 1).wait_recv()
        else:
            z_across(k, s2_r.at[k]).wait_recv()

    def activations(k):
        gx[k] = activation(k, 1)
        gall[dp * NK + k, own_g, :] = activation(k, 0)

    def ga(k, x):
        return ga_r.at[(k // 2 * 2 if k < NK - 2 else 2 * k - NK + 2) + x]

    def activation_send(k):
        x_copy(6, ha_r.at[k], k, emb=across).start()
        x_copy(5, hs_r.at[k], k).start()
        if k >= DIRECT:
            x_copy(9, ga(k, 1), k, emb=corner).start()
            x_copy(10, ga(k, 1), k, emb=partner).start()
        g_copy(2, gy_r.at[k], dp, own_g, k, emb=across).start()
        g_copy(3, ga(k, 0), dp, own_g, k, emb=partner).start()
        if k >= DIRECT:
            g_copy(11, ga(k, 0), dp, own_g, k, emb=corner).start()

    def stage_c(k):
        activation_wait(k)
        activations(k)
        activation_send(k)

    def logits_sum():
        logit_pair().wait_recv()
        lsnd2[...] = lbuf[mine, :] + lrecv1[mine, :]
        logit_across().start()

    gather_own(0)
    products(0, 0)
    logits_sum()

    c_copy().wait_recv()
    slots(cx_ref, posx_ref)

    def buildx(b, carry):
        at = pl.multiple_of(dp * NK * EB + b * 2 * EB, 2 * EB)
        ohx[b] = hot_rows(posx_ref[pl.ds(at, 2 * EB), :]).astype(BF)
        return carry

    lax.fori_loop(0, NK // 2, buildx, 0)
    stage_b(0, 0)
    remote(sq_snd, sq_recv.at[pl.ds(3, 4)], sq_s, sq_r.at[1], dp=xp).wait_recv()
    h_copy().wait_recv()
    bother[...] = normed(hx_ref, functools.reduce(lax.add, [sq_recv[n] for n in range(3, 7)]))
    gather_other(0)

    def from_across(k):
        return g_copy(2, gy_r.at[k], dp, other_g, k, emb=across)

    def from_x(k, rows, r):
        return g_copy(5, r, xp, rows, k, dp=xp)

    def stage_d(k):
        from_across(k).wait_recv()
        g_copy(4, ga(k, 0), dp, other_g, k, emb=partner).start()
        from_x(k, own_g, hs_r.at[k]).wait_recv()
        g_copy(7, ga(k, 1), xp, own_g, k, emb=partner).start()
        from_x(k, other_g, ha_r.at[k]).wait_recv()
        g_copy(8, ga(k, 1), xp, other_g, k, emb=partner).start()

    hw = width // 2
    both, first, second = slice(0, width), slice(0, hw), slice(hw, width)

    def combine(n, cols):
        macc[:, cols] += jnp.dot(oh[pair_no(n)], ubuf[n % 2, :, cols], preferred_element_type=F32)

    def arrived(n):
        w2_copy(n).wait()
        g_copy(3, ga_r.at[n], dp if n % 2 == 0 else xp, theirs, n // 2 * 2, 2, emb=partner).wait_recv()

    def expert_out(b, e, hot, prob, buf, to, cols):
        q, w = e // 2, e % 2
        gate = jnp.sum(hot.astype(F32) * prob, axis=1, keepdims=True)
        low = gall[b, q * QUART + w * CAP:q * QUART + (w + 1) * CAP, :]
        high = gall[b, q * QUART + 2 * CAP:(q + 1) * QUART, w * 64:(w + 1) * 64]
        y = jnp.dot(jnp.concatenate([low, high], axis=1), w2buf[b * EB + e, :, cols], preferred_element_type=F32)
        ubuf[buf % 2, to:to + CAP, cols] = (y.astype(BF).astype(F32) * gate).astype(BF)

    def down(n, cols):
        p = pair_no(n)
        probs = pt_ref[pl.ds(pl.multiple_of(p * 2 * EB, 2 * EB), 2 * EB), :]
        for e in range(2 * EB):
            expert_out(2 * p + e // EB, e % EB, oht[p, e * CAP:(e + 1) * CAP, :], probs[e:e + 1, :], n, e * CAP, cols)

    def arrived_last(k):
        if k >= DIRECT:
            from_across(k).wait_recv()
            from_x(k, own_g, hs_r.at[k]).wait_recv()
            from_x(k, other_g, ha_r.at[k]).wait_recv()
        for x, half_no in ((0, dp), (1, xp)):
            g_copy(3, ga(k, x), half_no, theirs, k, emb=partner).wait_recv()

    def down_last(k, cols):
        for x, half_no in ((0, dp), (1, xp)):
            p = half_no * (NK // 2) + k // 2
            probs = pt_ref[pl.ds(pl.multiple_of((half_no * NK + k) * EB, EB), EB), :]
            for e in range(EB):
                at = (k % 2 * EB + e) * CAP
                expert_out(half_no * NK + k, e, oht[p, at:at + CAP, :], probs[e:e + 1, :], k, (x * EB + e) * CAP, cols)

    def combine_last(k, cols):
        part_k = slice(k % 2 * rows_k, (k % 2 + 1) * rows_k)
        for x, half_no in ((0, dp), (1, xp)):
            hot = oh[half_no * (NK // 2) + k // 2, :, part_k]
            macc[:, cols] += jnp.dot(hot, ubuf[k % 2, x * rows_k:(x + 1) * rows_k, cols], preferred_element_type=F32)

    def down_both(n):
        arrived(n)
        if n:
            combine(n - 1, both)
        down(n, both)

    def probabilities():
        logit_across().wait_recv()
        logits = lsnd2[...] + lrecv2[...]
        pbuf[mine, :] = jax.nn.softmax(logits, axis=1)
        prob_pair().start()

    def gates():
        prob_pair().wait_recv()
        pt_ref[...] = jnp.transpose(pbuf[...])

    products(0, 1)
    products(1)
    stage_b(0, 1)
    products(2)
    stage_b(1)
    products(3)
    stage_b(2)
    products(4, act=0)
    stage_b(3)
    probabilities()
    products(5, act=1)
    stage_b(4)
    products(6, act=2)
    stage_b(5)
    gates()
    products(7)
    stage_b(6)
    stage_d(0)
    stage_c(3)
    stage_b(7)
    stage_c(4)
    stage_d(1)
    stage_c(5)
    down_both(0)
    stage_d(2)
    stage_c(6)
    down_both(1)
    stage_d(3)
    stage_c(7)
    stage_d(4)
    down_both(2)
    stage_d(5)
    down_both(3)
    stage_d(6)
    down_both(4)
    down_both(5)
    combine(5, both)
    w2_copy(6).wait()
    w2_copy(7).wait()
    arrived_last(6)
    down_last(6, both)
    combine_last(6, both)

    part = tok // 4

    def rs_copy(d, col):
        peer = (ffn + d) % 4
        cols = pl.ds(col * hw, hw)
        return remote(macc.at[pl.ds(pl.multiple_of(peer * part, part), part), cols], mrecv.at[d - 1, :, cols],
                      rs_s, rs_r.at[col], ffn=peer)

    arrived_last(7)
    down_last(7, first)
    combine_last(7, first)
    for d in (2, 1, 3):
        rs_copy(d, 0).start()
    down_last(7, second)
    combine_last(7, second)
    for d in (2, 1, 3):
        rs_copy(d, 1).start()

    my_tok = pl.ds(pl.multiple_of(ffn * part, part), part)
    for c in (z_pair, z_across):
        c(every, s1_r.at[0]).wait_send()
    for sem, x, rows, k, count in ((2, dp, own_g, 0, NK), (3, dp, own_g, 0, NK), (4, dp, other_g, 0, DIRECT),
                                   (7, xp, own_g, 0, DIRECT), (8, xp, other_g, 0, DIRECT), (11, dp, own_g, DIRECT, NK - DIRECT)):
        g_copy(sem, gy_r.at[0], x, rows, k, count, emb=partner).wait_send()
    for sem, k, count in ((5, 0, NK), (6, 0, NK), (9, DIRECT, NK - DIRECT), (10, DIRECT, NK - DIRECT)):
        x_copy(sem, gy_r.at[0], k, count).wait_send()
    h_copy().wait_send()
    c_copy().wait_send()
    remote(sq_recv, sq_recv, sq_s, sq_r.at[0], dp=xp).wait_send()
    logit_pair().wait_send()
    logit_across().wait_send()
    prob_pair().wait_send()
    m = macc[my_tok, :]
    for col in range(2):
        all_in = mrecv.at[:, :, pl.ds(col * hw, hw)]
        remote(all_in, all_in, rs_s, rs_r.at[col], ffn=(ffn + 1) % 4).wait_recv()
    for d in range(1, 4):
        m = m + mrecv[d - 1]
    mown[...] = m
    m2 = m * m
    tq_snd[...] = functools.reduce(lax.add, jnp.split(m2, width // LANES, axis=1))

    def tq_copy(d):
        return remote(tq_snd, tq_recv.at[d - 1], tq_s, tq_r, emb=(emb + d) % 4)

    for d in (2, 3, 1):
        tq_copy(d).start()
    remote(mrecv, mrecv, rs_s, rs_r.at[0], ffn=(ffn + 1) % 4).wait_send()
    remote(tq_recv, tq_recv, tq_s, tq_r, emb=partner).wait()
    tot = tq_snd[...]
    for d in range(1, 4):
        tot = tot + tq_recv[d - 1]
    inv_post = lax.rsqrt(jnp.sum(tot, axis=1, keepdims=True) / model_width + EPS)
    res = h_ref[my_tok, :].astype(F32) + mown[...] * inv_post * post_ref[...].astype(F32).reshape(1, -1)
    obuf[...] = res.astype(BF)

    def ag_copy(d):
        return remote(obuf, o_ref.at[my_tok], ag_s, ag_r, ffn=(ffn + d) % 4)

    for d in (2, 1, 3):
        ag_copy(d).start()
    keep = pltpu.make_async_copy(obuf, o_ref.at[my_tok], in_sem.at[0])
    keep.start()
    others = o_ref.at[pl.ds(0, 3 * part)]
    keep.wait()
    remote(others, others, ag_s, ag_r, ffn=(ffn + 1) % 4).wait()


def solution(mesh):
    emb_size = mesh.shape['emb']

    def local_block(hidden, norm_pre, norm_post, w_router, w_gate, w_up, w_down, choice):
        tok, width = hidden.shape
        experts, _, fw = w_gate.shape
        dma = one = pltpu.SemaphoreType.DMA
        vm = pltpu.VMEM
        rows = EB * CAP
        return pl.pallas_call(
            functools.partial(kernel, width * emb_size),
            out_shape=jax.ShapeDtypeStruct((tok, width), BF),
            in_specs=[pl.BlockSpec(memory_space=pl.ANY)] * 8,
            out_specs=pl.BlockSpec(memory_space=pl.ANY),
            scratch_shapes=[
                vm((tok, width), BF), vm((width,), BF), vm((width,), BF), vm((width, experts), BF), vm((8, tok), jnp.int32),
                vm((tok, width), BF), vm((8, tok), jnp.int32),
                vm((NK, EB, 2 * fw, width), BF), vm((experts, fw, width), BF),
                vm((NB // 2, 2 * rows, tok), BF), vm((NK // 2, 2 * rows, tok), BF), vm((NB // 2, tok, 2 * rows), BF),
                vm((tok, width), BF), vm((tok, width), BF),
                vm((NK, 2, rows, 2 * fw), BF), vm((NK, 2, rows // 2, 2 * fw), BF),
                vm((NK, 2, rows // 4, 2 * fw), BF), vm((NK, 2, rows // 4, 2 * fw), BF), vm((NK, 2, rows // 4, 2 * fw), F32),
                vm((NB, 4 * QUART, 128), BF), vm((NK, QUART, 128), BF),
                vm((experts, tok), F32), vm((experts, tok), F32), vm((experts, tok), F32),
                vm((tok, experts), F32), vm((tok, experts), F32), vm((tok // 2, experts), F32),
                vm((tok // 2, experts), F32), vm((tok, experts), F32),
                vm((8, tok), F32), vm((7, 8, tok), F32),
                vm((tok, width), F32), vm((2, 2 * rows, width), BF), vm((3, tok // 4, width), F32), vm((tok // 4, width), F32),
                vm((tok // 4, 128), F32), vm((3, tok // 4, 128), F32), vm((tok // 4, width), BF), vm((2, 2, rows, width), BF),
                dma((5,)), dma((NK,)), dma((12,)), dma((NK + 1,)), dma((NK + 1,)), dma((NK,)), dma((NK,)), dma((NK,)), dma((NK + 2,)),
                dma((3,)), dma((3,)), dma((2,)), dma((2,)), one, dma((2,)),
                one, dma((2,)), one, one, one, one,
            ],
            compiler_params=pltpu.CompilerParams(
                collective_id=0, has_side_effects=True, vmem_limit_bytes=67043328),
        )(hidden, norm_pre, norm_post, w_router, choice.T,
          jnp.swapaxes(w_gate, 1, 2), jnp.swapaxes(w_up, 1, 2), w_down)

    in_specs = (P('dp', 'emb'), P('emb'), P('emb'), P('emb', None), P(None, 'emb', 'ffn'), P(None, 'emb', 'ffn'), P(None, 'ffn', 'emb'), P('dp', None))
    return jax.shard_map(local_block, mesh=mesh, in_specs=in_specs, out_specs=P('dp', 'emb'), check_vma=False)
```

```python
import functools

import jax
import jax.numpy as jnp
from jax import lax
from jax.experimental import pallas as pl
from jax.experimental.pallas import tpu as pltpu
from jax.sharding import PartitionSpec as P

EPS = 1e-5
MESH = pl.DeviceIdType.MESH
BF = jnp.bfloat16
F32 = jnp.float32
LANES = 128
EB = 8
CAP = 16
NK = 8
NB = 16
DIRECT = 7
QUART = 48


def remote(src, dst, send, recv, **where):
    return pltpu.make_async_remote_copy(
        src_ref=src, dst_ref=dst, send_sem=send, recv_sem=recv,
        device_id=where, device_id_type=MESH)


def kernel(model_width, h_hbm, pre_hbm, post_hbm, wr_hbm, choice_hbm, w0_ref, w1_ref, w2_ref, o_ref,
           h_ref, pre_ref, post_ref, wr_ref, choice_ref, hx_ref, cx_ref,
           w01, w2buf, oht, ohx, oh, bnorm, bother, zsend, recv1, snd2, recv2, own2, gall, gx, pos_ref, posx_ref, pt_ref,
           lbuf, lrecv1, lsnd2, lrecv2, pbuf, sq_snd, sq_recv, macc, ubuf, mrecv, mown, tq_snd, tq_recv, obuf, xbuf,
           in_sem, w_sem, snd_sem, s1_r, s2_r, gy_r, hs_r, ha_r, ga_r,
           l_s, l_r, x_s, x_r, sq_s, sq_r, rs_s, rs_r, tq_s, tq_r, ag_s, ag_r):
    dp = lax.axis_index("dp")
    ffn = lax.axis_index("ffn")
    emb = lax.axis_index("emb")
    xp = 1 - dp
    core = emb % 2
    row = emb // 2
    partner = emb + 1 - 2 * core
    across = (emb + 2) % 4
    tok, width = h_ref.shape
    half = EB * CAP // 2
    quarter = half // 2

    barrier = pltpu.get_barrier_semaphore()
    for d in range(1, 4):
        pl.semaphore_signal(barrier, inc=1, device_id={"ffn": (ffn + d) % 4}, device_id_type=MESH)
        pl.semaphore_signal(barrier, inc=1, device_id={"emb": (emb + d) % 4}, device_id_type=MESH)
    for d in range(4):
        pl.semaphore_signal(barrier, inc=1, device_id={"dp": xp, "emb": (emb + d) % 4}, device_id_type=MESH)

    loads = [pltpu.make_async_copy(a, b, in_sem.at[n]) for n, (a, b) in enumerate(
        [(h_hbm, h_ref), (choice_hbm, choice_ref), (pre_hbm, pre_ref), (wr_hbm, wr_ref), (post_hbm, post_ref)])]
    for c in loads:
        c.start()

    def w01_start(k):
        e0 = pl.ds((dp * NK + k) * EB, EB)
        pltpu.make_async_copy(w0_ref.at[e0, pl.ds(0, 128)], w01.at[k, :, pl.ds(0, 128)], w_sem.at[k]).start()
        pltpu.make_async_copy(w1_ref.at[e0, pl.ds(0, 128)], w01.at[k, :, pl.ds(128, 128)], w_sem.at[k]).start()
        pltpu.make_async_copy(w0_ref.at[e0, pl.ds(128, 64)], w01.at[k, :, pl.ds(256, 64)], w_sem.at[k]).start()
        pltpu.make_async_copy(w1_ref.at[e0, pl.ds(128, 64)], w01.at[k, :, pl.ds(320, 64)], w_sem.at[k]).start()

    def w01_wait(k):
        pltpu.make_async_copy(w01.at[k], w01.at[k], w_sem.at[k]).wait()

    def pair_no(n):
        return (dp if n % 2 == 0 else xp) * (NK // 2) + n // 2

    def w2_copy(n):
        e0 = pl.ds(pair_no(n) * 2 * EB, 2 * EB)
        return pltpu.make_async_copy(w2_ref.at[e0], w2buf.at[e0], w_sem.at[n])

    for c in loads:
        c.wait()
    pl.semaphore_wait(barrier, 10)

    def sq_copy(n):
        where = dict(emb=(emb + n + 1) % 4) if n < 3 else dict(dp=xp, emb=(emb + n - 3) % 4)
        return remote(sq_snd, sq_recv.at[n], sq_s, sq_r.at[0 if n < 3 else 1], **where)

    def h_copy():
        return remote(h_ref, hx_ref, x_s.at[0], x_r.at[0], dp=xp)

    def c_copy():
        return remote(choice_ref, cx_ref, x_s.at[1], x_r.at[1], dp=xp)

    c_copy().start()
    h_copy().start()

    hf = h_ref[...].astype(F32)
    sq = jnp.sum(hf * hf, axis=1, keepdims=True)
    sq_snd[...] = jnp.transpose(jnp.broadcast_to(sq, (tok, tok)))[0:8]
    for n in range(7):
        sq_copy(n).start()
    for k in range(NK):
        w01_start(k)

    experts = lax.broadcasted_iota(jnp.int32, (tok, tok), 0)
    lanes = lax.broadcasted_iota(jnp.int32, (tok, tok), 1)
    upper = (experts < lanes).astype(F32).astype(BF)
    slot_no = lax.broadcasted_iota(jnp.int32, (CAP, tok), 0).astype(F32)

    def slots(choices, out):
        assigned = jnp.zeros((tok, tok), F32)
        for k in range(choices.shape[0]):
            assigned = assigned + (jnp.broadcast_to(choices[k:k + 1, :], (tok, tok)) == experts).astype(F32)
        before = jnp.dot(assigned.astype(BF), upper, preferred_element_type=F32)
        out[...] = jnp.where(assigned > 0.5, before, 1000.0)

    def hot_rows(rows):
        return jnp.concatenate(
            [(jnp.broadcast_to(rows[e:e + 1, :], (CAP, tok)) == slot_no).astype(F32) for e in range(2 * EB)], axis=0)

    slots(choice_ref, pos_ref)

    def build(b, carry):
        hot = hot_rows(pos_ref[pl.ds(pl.multiple_of(b * 2 * EB, 2 * EB), 2 * EB), :])
        oht[b] = hot.astype(BF)
        oh[b] = jnp.transpose(hot).astype(BF)
        return carry

    lax.fori_loop(0, NB // 2, build, 0)
    macc[...] = jnp.zeros_like(macc)

    def normed(x, total):
        inv_rows = lax.rsqrt(total / model_width + EPS)
        inv = jnp.transpose(jnp.broadcast_to(inv_rows[0:1, :], (tok, tok)))[:, 0:1]
        return (x[...].astype(F32) * inv * pre_ref[...].astype(F32).reshape(1, -1)).astype(BF)

    remote(sq_snd, sq_recv.at[pl.ds(0, 3)], sq_s, sq_r.at[0], emb=across).wait_recv()
    bnorm[...] = normed(h_ref, functools.reduce(lax.add, [sq_recv[n] for n in range(3)], sq_snd[...]))

    lbuf[...] = jnp.dot(bnorm[...], wr_ref[...], preferred_element_type=F32)
    htok = tok // 2
    mine = pl.ds(pl.multiple_of(core * htok, htok), htok)

    def logit_pair():
        return remote(lbuf, lrecv1, l_s.at[0], l_r.at[0], emb=partner)

    def logit_across():
        return remote(lsnd2, lrecv2, l_s.at[1], l_r.at[1], emb=across)

    def prob_pair():
        return remote(pbuf.at[mine], pbuf.at[mine], l_s.at[2], l_r.at[2], emb=partner)

    logit_pair().start()

    own_rows = pl.ds(pl.multiple_of(core * half + row * quarter, quarter), quarter)
    other_rows = pl.ds(pl.multiple_of(core * half + (1 - row) * quarter, quarter), quarter)
    pair_rows = pl.ds(pl.multiple_of((1 - core) * half, half), half)
    own_g = pl.ds(pl.multiple_of((core * 2 + row) * QUART, 16), QUART)
    other_g = pl.ds(pl.multiple_of((core * 2 + 1 - row) * QUART, 16), QUART)

    every = slice(None)

    def z_pair(k, r, g=every):
        return remote(zsend.at[k, g, pair_rows], recv1.at[k, g], snd_sem.at[0], r, emb=partner)

    def z_across(k, r, g=every):
        return remote(snd2.at[k, g], recv2.at[k, g], snd_sem.at[1], r, emb=across)

    def g_at(x, k, rows, count=None):
        return gall.at[x * NK + k if count is None else pl.ds(x * NK + k, count), rows]

    def g_copy(sem, r, x, rows, k, count=None, **where):
        return remote(g_at(x, k, rows, count), g_at(x, k, rows, count), snd_sem.at[sem], r, **where)

    def x_copy(sem, r, k, count=None, **where):
        return remote(gx.at[k if count is None else pl.ds(k, count)], g_at(dp, k, own_g, count), snd_sem.at[sem], r, dp=xp, **where)

    theirs = pl.ds(pl.multiple_of((1 - core) * 2 * QUART, 16), 2 * QUART)
    corner = 3 - emb

    rows_k = EB * CAP

    def gather_own(k):
        part_k = slice(k % 2 * rows_k, (k % 2 + 1) * rows_k)
        x = jnp.dot(oht[dp * (NK // 2) + k // 2, part_k, :], bnorm[...], preferred_element_type=F32)
        xbuf[k % 2, 0] = x.astype(BF)

    def gather_other(k):
        part_k = slice(k % 2 * rows_k, (k % 2 + 1) * rows_k)
        x = jnp.dot(ohx[k // 2, part_k, :], bother[...], preferred_element_type=F32)
        xbuf[k % 2, 1] = x.astype(BF)

    def products(k, g=every, act=None):
        if act is not None:
            activation_wait(act)
        if g != 1:
            w01_wait(k)
        for e in range(EB):
            rows = slice(e * CAP, (e + 1) * CAP)
            if g == every:
                x = jnp.concatenate([xbuf[k % 2, 0, rows, :], xbuf[k % 2, 1, rows, :]], axis=0)
            else:
                x = xbuf[k % 2, g, rows, :]
            z = lax.dot_general(x, w01[k, e], (((1,), (1,)), ((), ())), preferred_element_type=F32).astype(BF)
            if g != 1:
                zsend[k, 0, rows, :] = z[0:CAP]
            if g != 0:
                zsend[k, 1, rows, :] = z[-CAP:]
        if g != 0 and k + 1 < NK:
            gather_own(k + 1)
            gather_other(k + 1)
        if act is not None:
            activations(act)
        z_pair(k, s1_r.at[NK if g == 1 else k], g).start()
        if act is not None:
            activation_send(act)
        if g != 0:
            w2_copy(k).start()

    def stage_b(k, g=every):
        z_pair(k, s1_r.at[NK if g == 1 else k], g).wait_recv()
        near = pl.ds(pl.multiple_of(row * quarter, quarter), quarter)
        far = pl.ds(pl.multiple_of((1 - row) * quarter, quarter), quarter)
        snd2[k, g] = (zsend[k, g, other_rows, :].astype(F32) + recv1[k, g, far, :].astype(F32)).astype(BF)
        z_across(k, s2_r.at[NK if g == 1 else k], g).start()
        own2[k, g] = zsend[k, g, own_rows, :].astype(F32) + recv1[k, g, near, :].astype(F32)

    low_lane = lax.broadcasted_iota(jnp.int32, (CAP, 128), 1) < 64

    def activation(k, g):
        z = (own2[k, g] + recv2[k, g].astype(F32)).astype(BF).astype(F32)
        low = (jax.nn.gelu(z[:, 0:128], approximate=True) * z[:, 128:256]).astype(BF)
        mixed = z[:, 256:384]
        high = jax.nn.gelu(mixed, approximate=True) * pltpu.roll(mixed, 64, 1)
        packed = jnp.where(low_lane, high[0:CAP], pltpu.roll(high[CAP:], 64, 1)).astype(BF)
        return jnp.concatenate([low, packed], axis=0)

    def activation_wait(k):
        if k == 0:
            z_across(0, s2_r.at[0], 0).wait_recv()
            z_across(0, s2_r.at[NK], 1).wait_recv()
        else:
            z_across(k, s2_r.at[k]).wait_recv()

    def activations(k):
        gx[k] = activation(k, 1)
        gall[dp * NK + k, own_g, :] = activation(k, 0)

    def ga(k, x):
        return ga_r.at[(k // 2 * 2 if k < NK - 2 else 2 * k - NK + 2) + x]

    def activation_send(k):
        x_copy(6, ha_r.at[k], k, emb=across).start()
        x_copy(5, hs_r.at[k], k).start()
        if k >= DIRECT:
            x_copy(9, ga(k, 1), k, emb=corner).start()
            x_copy(10, ga(k, 1), k, emb=partner).start()
        g_copy(2, gy_r.at[k], dp, own_g, k, emb=across).start()
        g_copy(3, ga(k, 0), dp, own_g, k, emb=partner).start()
        if k >= DIRECT:
            g_copy(11, ga(k, 0), dp, own_g, k, emb=corner).start()

    def stage_c(k):
        activation_wait(k)
        activations(k)
        activation_send(k)

    def logits_sum():
        logit_pair().wait_recv()
        lsnd2[...] = lbuf[mine, :] + lrecv1[mine, :]
        logit_across().start()

    gather_own(0)
    products(0, 0)
    logits_sum()

    c_copy().wait_recv()
    slots(cx_ref, posx_ref)

    def buildx(b, carry):
        at = pl.multiple_of(dp * NK * EB + b * 2 * EB, 2 * EB)
        ohx[b] = hot_rows(posx_ref[pl.ds(at, 2 * EB), :]).astype(BF)
        return carry

    lax.fori_loop(0, NK // 2, buildx, 0)
    stage_b(0, 0)
    remote(sq_snd, sq_recv.at[pl.ds(3, 4)], sq_s, sq_r.at[1], dp=xp).wait_recv()
    h_copy().wait_recv()
    bother[...] = normed(hx_ref, functools.reduce(lax.add, [sq_recv[n] for n in range(3, 7)]))
    gather_other(0)

    def from_across(k):
        return g_copy(2, gy_r.at[k], dp, other_g, k, emb=across)

    def from_x(k, rows, r):
        return g_copy(5, r, xp, rows, k, dp=xp)

    def stage_d(k):
        from_across(k).wait_recv()
        g_copy(4, ga(k, 0), dp, other_g, k, emb=partner).start()
        from_x(k, own_g, hs_r.at[k]).wait_recv()
        g_copy(7, ga(k, 1), xp, own_g, k, emb=partner).start()
        from_x(k, other_g, ha_r.at[k]).wait_recv()
        g_copy(8, ga(k, 1), xp, other_g, k, emb=partner).start()

    hw = width // 2
    both, first, second = slice(0, width), slice(0, hw), slice(hw, width)

    def combine(n, cols):
        macc[:, cols] += jnp.dot(oh[pair_no(n)], ubuf[n % 2, :, cols], preferred_element_type=F32)

    def arrived(n):
        w2_copy(n).wait()
        g_copy(3, ga_r.at[n], dp if n % 2 == 0 else xp, theirs, n // 2 * 2, 2, emb=partner).wait_recv()

    def expert_out(b, e, hot, prob, buf, to, cols):
        q, w = e // 2, e % 2
        gate = jnp.sum(hot.astype(F32) * prob, axis=1, keepdims=True)
        low = gall[b, q * QUART + w * CAP:q * QUART + (w + 1) * CAP, :]
        high = gall[b, q * QUART + 2 * CAP:(q + 1) * QUART, w * 64:(w + 1) * 64]
        y = jnp.dot(jnp.concatenate([low, high], axis=1), w2buf[b * EB + e, :, cols], preferred_element_type=F32)
        ubuf[buf % 2, to:to + CAP, cols] = (y.astype(BF).astype(F32) * gate).astype(BF)

    def down(n, cols):
        p = pair_no(n)
        probs = pt_ref[pl.ds(pl.multiple_of(p * 2 * EB, 2 * EB), 2 * EB), :]
        for e in range(2 * EB):
            expert_out(2 * p + e // EB, e % EB, oht[p, e * CAP:(e + 1) * CAP, :], probs[e:e + 1, :], n, e * CAP, cols)

    def arrived_last(k):
        if k >= DIRECT:
            from_across(k).wait_recv()
            from_x(k, own_g, hs_r.at[k]).wait_recv()
            from_x(k, other_g, ha_r.at[k]).wait_recv()
        for x, half_no in ((0, dp), (1, xp)):
            g_copy(3, ga(k, x), half_no, theirs, k, emb=partner).wait_recv()

    def down_last(k, cols):
        for x, half_no in ((0, dp), (1, xp)):
            p = half_no * (NK // 2) + k // 2
            probs = pt_ref[pl.ds(pl.multiple_of((half_no * NK + k) * EB, EB), EB), :]
            for e in range(EB):
                at = (k % 2 * EB + e) * CAP
                expert_out(half_no * NK + k, e, oht[p, at:at + CAP, :], probs[e:e + 1, :], k, (x * EB + e) * CAP, cols)

    def combine_last(k, cols):
        part_k = slice(k % 2 * rows_k, (k % 2 + 1) * rows_k)
        for x, half_no in ((0, dp), (1, xp)):
            hot = oh[half_no * (NK // 2) + k // 2, :, part_k]
            macc[:, cols] += jnp.dot(hot, ubuf[k % 2, x * rows_k:(x + 1) * rows_k, cols], preferred_element_type=F32)

    def down_both(n):
        arrived(n)
        if n:
            combine(n - 1, both)
        down(n, both)

    def probabilities():
        logit_across().wait_recv()
        logits = lsnd2[...] + lrecv2[...]
        pbuf[mine, :] = jax.nn.softmax(logits, axis=1)
        prob_pair().start()

    def gates():
        prob_pair().wait_recv()
        pt_ref[...] = jnp.transpose(pbuf[...])

    products(0, 1)
    products(1)
    stage_b(0, 1)
    products(2)
    stage_b(1)
    products(3)
    stage_b(2)
    products(4, act=0)
    stage_b(3)
    probabilities()
    products(5, act=1)
    stage_b(4)
    products(6, act=2)
    stage_b(5)
    gates()
    products(7)
    stage_b(6)
    stage_d(0)
    stage_c(3)
    stage_b(7)
    stage_c(4)
    stage_d(1)
    stage_c(5)
    down_both(0)
    stage_d(2)
    stage_c(6)
    down_both(1)
    stage_d(3)
    stage_c(7)
    stage_d(4)
    down_both(2)
    stage_d(5)
    down_both(3)
    stage_d(6)
    down_both(4)
    down_both(5)
    combine(5, both)
    w2_copy(6).wait()
    w2_copy(7).wait()
    arrived_last(6)
    down_last(6, both)
    combine_last(6, both)

    part = tok // 4

    def rs_copy(d, col):
        peer = (ffn + d) % 4
        cols = pl.ds(col * hw, hw)
        return remote(macc.at[pl.ds(pl.multiple_of(peer * part, part), part), cols], mrecv.at[d - 1, :, cols],
                      rs_s, rs_r.at[col], ffn=peer)

    arrived_last(7)
    down_last(7, first)
    combine_last(7, first)
    for d in (2, 1, 3):
        rs_copy(d, 0).start()
    down_last(7, second)
    combine_last(7, second)
    for d in (2, 1, 3):
        rs_copy(d, 1).start()

    my_tok = pl.ds(pl.multiple_of(ffn * part, part), part)
    for c in (z_pair, z_across):
        c(every, s1_r.at[0]).wait_send()
    for sem, x, rows, k, count in ((2, dp, own_g, 0, NK), (3, dp, own_g, 0, NK), (4, dp, other_g, 0, DIRECT),
                                   (7, xp, own_g, 0, DIRECT), (8, xp, other_g, 0, DIRECT), (11, dp, own_g, DIRECT, NK - DIRECT)):
        g_copy(sem, gy_r.at[0], x, rows, k, count, emb=partner).wait_send()
    for sem, k, count in ((5, 0, NK), (6, 0, NK), (9, DIRECT, NK - DIRECT), (10, DIRECT, NK - DIRECT)):
        x_copy(sem, gy_r.at[0], k, count).wait_send()
    h_copy().wait_send()
    c_copy().wait_send()
    remote(sq_recv, sq_recv, sq_s, sq_r.at[0], dp=xp).wait_send()
    logit_pair().wait_send()
    logit_across().wait_send()
    prob_pair().wait_send()
    squares = []
    for col, cols in enumerate((first, second)):
        all_in = mrecv.at[:, :, pl.ds(col * hw, hw)]
        remote(all_in, all_in, rs_s, rs_r.at[col], ffn=(ffn + 1) % 4).wait_recv()
        m = functools.reduce(lax.add, [mrecv[d, :, cols] for d in range(3)], macc[my_tok, cols])
        mown[:, cols] = m
        squares += jnp.split(m * m, hw // LANES, axis=1)
    tq_snd[...] = functools.reduce(lax.add, squares)

    def tq_copy(d):
        return remote(tq_snd, tq_recv.at[d - 1], tq_s, tq_r, emb=(emb + d) % 4)

    for d in (2, 3, 1):
        tq_copy(d).start()
    remote(mrecv, mrecv, rs_s, rs_r.at[0], ffn=(ffn + 1) % 4).wait_send()
    remote(tq_recv, tq_recv, tq_s, tq_r, emb=partner).wait()
    tot = tq_snd[...]
    for d in range(1, 4):
        tot = tot + tq_recv[d - 1]
    inv_post = lax.rsqrt(jnp.sum(tot, axis=1, keepdims=True) / model_width + EPS)
    res = h_ref[my_tok, :].astype(F32) + mown[...] * inv_post * post_ref[...].astype(F32).reshape(1, -1)
    obuf[...] = res.astype(BF)

    def ag_copy(d):
        return remote(obuf, o_ref.at[my_tok], ag_s, ag_r, ffn=(ffn + d) % 4)

    for d in (2, 1, 3):
        ag_copy(d).start()
    keep = pltpu.make_async_copy(obuf, o_ref.at[my_tok], in_sem.at[0])
    keep.start()
    others = o_ref.at[pl.ds(0, 3 * part)]
    keep.wait()
    remote(others, others, ag_s, ag_r, ffn=(ffn + 1) % 4).wait()


def solution(mesh):
    emb_size = mesh.shape['emb']

    def local_block(hidden, norm_pre, norm_post, w_router, w_gate, w_up, w_down, choice):
        tok, width = hidden.shape
        experts, _, fw = w_gate.shape
        dma = one = pltpu.SemaphoreType.DMA
        vm = pltpu.VMEM
        rows = EB * CAP
        return pl.pallas_call(
            functools.partial(kernel, width * emb_size),
            out_shape=jax.ShapeDtypeStruct((tok, width), BF),
            in_specs=[pl.BlockSpec(memory_space=pl.ANY)] * 8,
            out_specs=pl.BlockSpec(memory_space=pl.ANY),
            scratch_shapes=[
                vm((tok, width), BF), vm((width,), BF), vm((width,), BF), vm((width, experts), BF), vm((8, tok), jnp.int32),
                vm((tok, width), BF), vm((8, tok), jnp.int32),
                vm((NK, EB, 2 * fw, width), BF), vm((experts, fw, width), BF),
                vm((NB // 2, 2 * rows, tok), BF), vm((NK // 2, 2 * rows, tok), BF), vm((NB // 2, tok, 2 * rows), BF),
                vm((tok, width), BF), vm((tok, width), BF),
                vm((NK, 2, rows, 2 * fw), BF), vm((NK, 2, rows // 2, 2 * fw), BF),
                vm((NK, 2, rows // 4, 2 * fw), BF), vm((NK, 2, rows // 4, 2 * fw), BF), vm((NK, 2, rows // 4, 2 * fw), F32),
                vm((NB, 4 * QUART, 128), BF), vm((NK, QUART, 128), BF),
                vm((experts, tok), F32), vm((experts, tok), F32), vm((experts, tok), F32),
                vm((tok, experts), F32), vm((tok, experts), F32), vm((tok // 2, experts), F32),
                vm((tok // 2, experts), F32), vm((tok, experts), F32),
                vm((8, tok), F32), vm((7, 8, tok), F32),
                vm((tok, width), F32), vm((2, 2 * rows, width), BF), vm((3, tok // 4, width), F32), vm((tok // 4, width), F32),
                vm((tok // 4, 128), F32), vm((3, tok // 4, 128), F32), vm((tok // 4, width), BF), vm((2, 2, rows, width), BF),
                dma((5,)), dma((NK,)), dma((12,)), dma((NK + 1,)), dma((NK + 1,)), dma((NK,)), dma((NK,)), dma((NK,)), dma((NK + 2,)),
                dma((3,)), dma((3,)), dma((2,)), dma((2,)), one, dma((2,)),
                one, dma((2,)), one, one, one, one,
            ],
            compiler_params=pltpu.CompilerParams(
                collective_id=0, has_side_effects=True, vmem_limit_bytes=67043328),
        )(hidden, norm_pre, norm_post, w_router, choice.T,
          jnp.swapaxes(w_gate, 1, 2), jnp.swapaxes(w_up, 1, 2), w_down)

    in_specs = (P('dp', 'emb'), P('emb'), P('emb'), P('emb', None), P(None, 'emb', 'ffn'), P(None, 'emb', 'ffn'), P(None, 'ffn', 'emb'), P('dp', None))
    return jax.shard_map(local_block, mesh=mesh, in_specs=in_specs, out_specs=P('dp', 'emb'), check_vma=False)
```
